256 devices in a mesh: groups: 2 (over z), cache: 16 (over x, core), tensor: 8 (over y).
Axes of the slice: x: 8, y: 8, z: 2, core: 2. Of those that a mesh axis runs over, the one named last changes fastest.
The devices are a block of a 8x8x16 slice.
Arguments:
- queries: bfloat16 [8192, 8192], P(('groups', 'cache'), 'tensor'), parts along dimension 0, may hold values from -8 to 8
- suffix_key_value: bfloat16 [2, 8192, 1024], P(None, ('groups', 'cache'), 'tensor'), parts along dimension 1, may hold values from -6 to 6
- kv_pages: bfloat16 [3072, 2, 128, 1024], P(('groups', 'cache'), None, None, 'tensor'), parts along dimension 0, may hold values from -6 to 6
- page_ids: int32 [32, 64], P(('groups', 'cache')), parts along dimension 0, may hold values from 0 to 1535, as said below
- prefix_pages: int32 [32], P(('groups', 'cache')), parts along dimension 0, may hold values from 8 to 64, as said below
- page_home: int32 [3072], P('groups'), parts along dimension 0, may hold values from 0 to 1535, as said below
- out_weight: bfloat16 [8192, 8192], P('tensor', 'cache'), may hold values from -0.25 to 0.25
Outputs:
- attended: bfloat16 [8192, 8192], P(('groups', 'cache'), 'tensor'), parts along dimension 0
The draws below stay inside these ranges and needn't reach their ends.
There are 2 independent parts, one for each index of `groups`. The reference program is written for one: setup_inputs(seed, part) draws one part's arguments, and reference() takes and returns one part's arrays. A program takes and returns all parts, laid end to end along the dimension named above; an argument that names none is the same for every part. Nothing has to cross between parts.
Inputs may be any that keep to these rules, and one draw needn't show every extreme that they name: `page_ids`: live slots are j < prefix_pages[r]. Within the aligned block of 1 request of one index of cache, no page id appears twice among all 64 slots, and at most 6 of these slots name pages whose row page_home[id] lies on one index of cache (row // 96); in every such block some index of cache gets exactly 6. `prefix_pages`: one request in each draw has 64 pages and another has 8. `page_home`: A permutation of 0 to 1535.
All inputs are finite; a program needn't handle non-finite values.
Results may differ from the reference program's by a relative error of at most 0.015.
Values may be sent and summed in bfloat16 or wider, within the bound.
A program may use at most 128 MiB of HBM per device.

```python
import jax
import jax.numpy as jnp
from jax import lax

D = 8192
QUERY_HEADS = 64
KEY_VALUE_HEADS = 8
HEAD_SIZE = 128
PAGE_TOKENS = 128
SUF = 256
MAXP = 64
MINP = 8
POOL_DEV = 96
REQ_DEV = 1
REQS = 16
NEW_TOKENS = 4096
STORED_PAGES = 1536
CAP = 6
N_CACHE = 16
N_TENSOR = 8


def page_layout(key):
    base_key = jax.random.fold_in(key, 7001)
    home_rows = jax.random.permutation(jax.random.fold_in(base_key, 1), STORED_PAGES).astype(jnp.int32)
    inverse = jnp.zeros((STORED_PAGES,), jnp.int32).at[home_rows].set(jnp.arange(STORED_PAGES, dtype=jnp.int32))
    slot_count = REQ_DEV * MAXP

    def one_device(device):
        device_key = jax.random.fold_in(base_key, 100 + device)
        remaining = jax.random.permutation(jax.random.fold_in(device_key, 1), N_CACHE * CAP - CAP).astype(jnp.int32) + CAP
        tickets = jnp.concatenate([jnp.arange(CAP, dtype=jnp.int32), remaining])[:slot_count]
        shuffle = jax.random.permutation(jax.random.fold_in(device_key, 2), slot_count)
        tickets = tickets[shuffle]
        first_owner = jax.random.randint(jax.random.fold_in(device_key, 3), (), 0, N_CACHE)
        owners = (tickets // CAP + first_owner) % N_CACHE
        offset = jax.random.randint(jax.random.fold_in(device_key, 4), (N_CACHE,), 0, POOL_DEV)
        within = (offset[owners] + tickets % CAP) % POOL_DEV
        return inverse[owners * POOL_DEV + within]
    page_list = jax.vmap(one_device)(jnp.arange(N_CACHE, dtype=jnp.int32))
    return (home_rows, page_list.reshape(N_CACHE * REQ_DEV, MAXP).astype(jnp.int32))


def draw_page_home(key, part):
    return page_layout(key)[0]


def draw_page_ids(key, part):
    return page_layout(key)[1]


def draw_prefix_pages(key, part):
    base_key = jax.random.fold_in(key, 7002)
    length_span = MAXP - MINP
    first_draw = jax.random.randint(jax.random.fold_in(base_key, 1), (REQS,), 0, length_span + 1)
    second_draw = jax.random.randint(jax.random.fold_in(base_key, 2), (REQS,), 0, length_span + 1)
    lengths = MAXP - first_draw * second_draw // max(length_span, 1)
    longest = jax.random.randint(jax.random.fold_in(base_key, 3), (), 0, REQS)
    step_away = jax.random.randint(jax.random.fold_in(base_key, 4), (), 1, max(REQS, 2))
    shortest = (longest + step_away) % REQS
    request_index = jnp.arange(REQS)
    lengths = jnp.where(request_index == shortest, MINP, lengths)
    lengths = jnp.where(request_index == longest, MAXP, lengths)
    return lengths.astype(jnp.int32)


def draw_queries(key, part):
    noise_key = jax.random.fold_in(key, 7004)
    values = jnp.clip(2.5 * jax.random.normal(noise_key, (NEW_TOKENS, QUERY_HEADS * HEAD_SIZE), jnp.float32), -8.0, 8.0)
    return values.astype(jnp.bfloat16)


def draw_kv_pages(key, part):
    noise_key = jax.random.fold_in(key, 7005)
    array_shape = (STORED_PAGES, 2, PAGE_TOKENS, KEY_VALUE_HEADS * HEAD_SIZE)
    values = jnp.clip(jax.random.normal(noise_key, array_shape, jnp.float32), -6.0, 6.0)
    return values.astype(jnp.bfloat16)


def steps_of(rng, extent, cuts, low, top_value):
    loudness, own = 1.0, jax.random.fold_in(rng, 6)
    for dim, parts in cuts:
        heights = jnp.exp(jax.random.uniform(jax.random.fold_in(own, dim), (parts,), jnp.float32, low / len(cuts), top_value / len(cuts)))
        loudness = loudness * jnp.repeat(heights, extent[dim] // parts).reshape([-1 if axis == dim else 1 for axis in range(len(extent))])
    return loudness


def gaussian(stream_key, extent, scale, most, shards=(), kind=jnp.bfloat16):
    result = scale * jax.random.normal(stream_key, extent, jnp.float32)
    if shards:
        result = result * steps_of(stream_key, extent, shards, -0.22, 0.18)
    return jnp.clip(result, -most, most).astype(kind)


def setup_inputs(seed: int = 0, part: int = 0) -> dict:
    streams_of = jax.random.split(jax.random.key(seed), 8)
    own_keys = jax.random.split(jax.random.fold_in(streams_of[7], part), 8)
    return {
        "queries": draw_queries(jax.random.fold_in(jax.random.fold_in(streams_of[7], part), 71), part),
        "suffix_key_value": gaussian(own_keys[1], (2, NEW_TOKENS, KEY_VALUE_HEADS * HEAD_SIZE), 1.0, 6.0, ((1, 16), (2, 8))),
        "kv_pages": draw_kv_pages(jax.random.fold_in(jax.random.fold_in(streams_of[7], part), 71), part),
        "page_ids": draw_page_ids(jax.random.fold_in(jax.random.fold_in(streams_of[7], part), 71), part),
        "prefix_pages": draw_prefix_pages(jax.random.fold_in(jax.random.fold_in(streams_of[7], part), 71), part),
        "page_home": draw_page_home(jax.random.fold_in(jax.random.fold_in(streams_of[7], part), 71), part),
        "out_weight": gaussian(streams_of[6], (QUERY_HEADS * HEAD_SIZE, D), (QUERY_HEADS * HEAD_SIZE // 16) ** -0.5, 0.25, ((0, 8), (1, 16))),
    }


def attend_head(query_head, key_rows, value_rows, allowed):
    scores = jnp.einsum("sgd,ld->sgl", query_head.astype(jnp.float32), key_rows.astype(jnp.float32)) * (HEAD_SIZE ** -0.5)
    scores = jnp.where(allowed[:, None, :], scores, -jnp.inf)
    row_top = jnp.max(scores, axis=2, keepdims=True)
    weights = jnp.where(allowed[:, None, :], jnp.exp(scores - row_top), 0.0)
    weight_sum = jnp.sum(weights, axis=2, keepdims=True)
    rounded = lax.optimization_barrier(weights.astype(jnp.bfloat16))
    accumulated = jnp.einsum("sgl,ld->sgd", rounded.astype(jnp.float32), value_rows.astype(jnp.float32))
    return (accumulated / weight_sum).astype(jnp.bfloat16)


def reference(queries, suffix_key_value, kv_pages, page_ids, prefix_pages, page_home, out_weight):
    group_width = QUERY_HEADS // KEY_VALUE_HEADS

    def one_request(request_index):
        page_list = page_ids[request_index]
        home_rows = jnp.take(page_home, page_list).astype(jnp.int32)
        pages_here = jnp.take(kv_pages, home_rows, axis=0)
        first_token = (request_index * SUF).astype(jnp.int32)
        query_rows = lax.dynamic_slice_in_dim(queries, first_token, SUF, 0)
        suffix_rows = lax.dynamic_slice_in_dim(suffix_key_value, first_token, SUF, 1)
        key_page = jnp.arange(MAXP * PAGE_TOKENS, dtype=jnp.int32) // PAGE_TOKENS
        prefix_live = jnp.broadcast_to((key_page < prefix_pages[request_index])[None, :], (SUF, MAXP * PAGE_TOKENS))
        positions = jnp.arange(SUF, dtype=jnp.int32)
        causal = positions[None, :] <= positions[:, None]
        allowed = jnp.concatenate([prefix_live, causal], axis=1)

        def single_head(head_index):
            query_head = lax.dynamic_slice_in_dim(query_rows, (head_index * group_width * HEAD_SIZE).astype(jnp.int32), group_width * HEAD_SIZE, 1)
            query_head = query_head.reshape(SUF, group_width, HEAD_SIZE)
            column = (head_index * HEAD_SIZE).astype(jnp.int32)
            prefix_keys = lax.dynamic_slice_in_dim(pages_here[:, 0], column, HEAD_SIZE, 2).reshape(MAXP * PAGE_TOKENS, HEAD_SIZE)
            prefix_values = lax.dynamic_slice_in_dim(pages_here[:, 1], column, HEAD_SIZE, 2).reshape(MAXP * PAGE_TOKENS, HEAD_SIZE)
            suffix_keys = lax.dynamic_slice_in_dim(suffix_rows[0], column, HEAD_SIZE, 1)
            suffix_values = lax.dynamic_slice_in_dim(suffix_rows[1], column, HEAD_SIZE, 1)
            key_rows = jnp.concatenate([prefix_keys, suffix_keys], axis=0)
            value_rows = jnp.concatenate([prefix_values, suffix_values], axis=0)
            return attend_head(query_head, key_rows, value_rows, allowed)

        head_list = lax.map(single_head, jnp.arange(KEY_VALUE_HEADS, dtype=jnp.int32))
        return jnp.transpose(head_list, (1, 0, 2, 3)).reshape(SUF, QUERY_HEADS * HEAD_SIZE)

    mixed_heads = lax.map(one_request, jnp.arange(REQS, dtype=jnp.int32)).reshape(NEW_TOKENS, QUERY_HEADS * HEAD_SIZE)
    span_cols = QUERY_HEADS * HEAD_SIZE // N_TENSOR
    summed = jnp.zeros((NEW_TOKENS, D), jnp.float32)
    for group_index in range(N_TENSOR):
        lower = group_index * span_cols
        group_term = jnp.dot(mixed_heads[:, lower:lower + span_cols], out_weight[lower:lower + span_cols], preferred_element_type=jnp.float32).astype(jnp.bfloat16)
        summed = summed + lax.optimization_barrier(group_term).astype(jnp.float32)
    return summed.astype(jnp.bfloat16)
```

```python
import functools

import jax
import jax.numpy as jnp
from jax import lax
from jax.experimental import pallas as pl
from jax.experimental.pallas import tpu as pltpu
from jax.sharding import Mesh
from jax.sharding import PartitionSpec as P

QUERY_HEADS = 64
KEY_VALUE_HEADS = 8
HEAD_SIZE = 128
PAGE_TOKENS = 128
SUF = 256
MAXP = 64
CACHE = ("cache_0", "cache_1")
GROUPS_CACHE = ("groups", "cache_0", "cache_1")
GROUP_WIDTH = QUERY_HEADS // KEY_VALUE_HEADS

LOG2_SCALE = HEAD_SIZE ** (-0.5) * 1.4426950408889634
DEAD = 1e30
HALF = SUF // 2
OUT_ROWS = GROUP_WIDTH * HEAD_SIZE
PART_ROWS = OUT_ROWS + 32
VALUE_ROWS = HEAD_SIZE + 16
MESH = pl.DeviceIdType.MESH


def joined_along(parts, dim):
    lengths = list(parts.shape[1:])
    lengths[dim] *= parts.shape[0]
    return jnp.moveaxis(parts, 0, dim).reshape(lengths)


def on_gathered_pieces(shard, axis, dim, apply, out_dim):
    peers, width = (lax.axis_size(axis), shard.shape[dim])
    count = 2 if width % 2 == 0 else 1
    finished, length = ([], width // count)
    for k in range(count):
        piece = lax.slice_in_dim(shard, k * length, (k + 1) * length, axis=dim)
        starts = jnp.arange(peers) * width + k * length
        finished.append(jax.vmap(apply)(lax.all_gather(piece, axis), starts))
    return joined_along(jnp.concatenate(finished, axis=out_dim + 1), out_dim)


def attention_kernel(
    capacity,
    chips,
    table,
    live,
    q_hbm,
    kv_hbm,
    suffix_hbm,
    out,
    pool,
    suffix,
    q_all,
    part,
    partner_part,
    ring_in,
    keys,
    values_t,
    scores,
    weights,
    tops,
    sums,
    local_sem,
    q_send,
    q_recv,
    q_core_send,
    q_core_recv,
    p_core_send,
    p_core_recv,
    p_send,
    p_recv,
):
    x = lax.axis_index("cache_0")
    core = lax.axis_index("cache_1")
    right = {"cache_0": lax.rem(x + 1, chips), "cache_1": core}
    left = {"cache_0": lax.rem(x + chips - 1, chips), "cache_1": core}
    partner = {"cache_0": x, "cache_1": 1 - core}
    far = chips // 2
    toward = (right, left)

    fetch_q = pltpu.make_async_copy(q_hbm, q_all.at[0, 0], local_sem.at[0])
    fetch_pool = pltpu.make_async_copy(kv_hbm, pool, local_sem.at[1])
    fetch_suffix = pltpu.make_async_copy(suffix_hbm, suffix, local_sem.at[2])
    fetch_q.start()
    fetch_pool.start()
    fetch_suffix.start()
    barrier = pltpu.get_barrier_semaphore()
    for peer in (right, left, partner):
        pl.semaphore_signal(barrier, inc=1, device_id=peer, device_id_type=MESH)
    values_t[HEAD_SIZE:, :] = jnp.ones((VALUE_ROWS - HEAD_SIZE, values_t.shape[1]), jnp.bfloat16)
    fetch_q.wait()
    pl.semaphore_wait(barrier, 3)

    def chunk(offset, kind, half):
        return q_all.at[offset % chips, kind, pl.ds(half * HALF, HALF), :]

    def q_copy(direction, step, half):
        sign = -1 if direction == 0 else 1
        return pltpu.make_async_remote_copy(
            src_ref=chunk(sign * (step - 1), 0, half),
            dst_ref=chunk(sign * step, 0, half),
            send_sem=q_send.at[direction, step - 1, half],
            recv_sem=q_recv.at[direction, step - 1, half],
            device_id=toward[direction],
            device_id_type=MESH,
        )

    def q_core_copy(offset, half):
        return pltpu.make_async_remote_copy(
            src_ref=chunk(offset, 0, half),
            dst_ref=chunk(offset, 1, half),
            send_sem=q_core_send.at[offset % chips, half],
            recv_sem=q_core_recv.at[offset % chips, half],
            device_id=partner,
            device_id_type=MESH,
        )

    def p_core_copy(offset):
        return pltpu.make_async_remote_copy(
            src_ref=part.at[offset % chips, 1],
            dst_ref=partner_part.at[offset % chips],
            send_sem=p_core_send.at[offset % chips],
            recv_sem=p_core_recv.at[offset % chips],
            device_id=partner,
            device_id_type=MESH,
        )

    def p_copy(direction, distance, half):
        sign = 1 if direction == 0 else -1
        return pltpu.make_async_remote_copy(
            src_ref=part.at[(sign * distance) % chips, 0, half],
            dst_ref=ring_in.at[direction, distance - 1, half],
            send_sem=p_send.at[direction, distance - 1, half],
            recv_sem=p_recv.at[direction, distance - 1, half],
            device_id=toward[direction],
            device_id_type=MESH,
        )

    def attend(offset, kind, own):
        where = offset % chips
        request = 2 * lax.rem(x + where, chips) + (core if kind == 0 else 1 - core)
        pages = capacity + (SUF // PAGE_TOKENS if own else 0)
        alive = []
        for j in range(capacity):
            row = table[request, j]
            alive.append(live[request, j])
            keys[j * PAGE_TOKENS : (j + 1) * PAGE_TOKENS, :] = pool[row, 0]
            values_t[0:HEAD_SIZE, j * PAGE_TOKENS : (j + 1) * PAGE_TOKENS] = pool[row, 1].T
        if own:
            keys[capacity * PAGE_TOKENS :, :] = suffix[0]
            values_t[0:HEAD_SIZE, capacity * PAGE_TOKENS :] = suffix[1].T

        def head(h, carry):
            q_head = q_all[where, kind, :, pl.ds(pl.multiple_of(h * HEAD_SIZE, HEAD_SIZE), HEAD_SIZE)]
            top = None
            for j in range(pages):
                span = pl.ds(j * PAGE_TOKENS, PAGE_TOKENS)
                piece = lax.dot_general(
                    keys[span, :], q_head, (((1,), (1,)), ((), ())), preferred_element_type=jnp.float32
                )
                if j >= capacity:
                    key_at = lax.broadcasted_iota(jnp.int32, piece.shape, 0) + (j - capacity) * PAGE_TOKENS
                    token_at = lax.broadcasted_iota(jnp.int32, piece.shape, 1)
                    piece = jnp.where(key_at <= token_at, piece, -DEAD)
                scores[span, :] = piece
                peak = jnp.max(piece, axis=0, keepdims=True)
                if j < capacity:
                    peak = peak * alive[j] + (alive[j] - 1.0) * DEAD
                top = peak if top is None else jnp.maximum(top, peak)
            level = jnp.ceil(top * (LOG2_SCALE * 0.25)) * 4.0
            for j in range(pages):
                span = pl.ds(j * PAGE_TOKENS, PAGE_TOKENS)
                shift = -level
                if j < capacity:
                    shift = shift * alive[j] + (alive[j] - 1.0) * DEAD
                weights[span, :] = jnp.exp2(scores[span, :] * LOG2_SCALE + shift).astype(jnp.bfloat16)
            length = pages * PAGE_TOKENS
            mixed = jnp.dot(values_t[:, 0:length], weights[0:length, :], preferred_element_type=jnp.float32)
            rows = pl.ds(pl.multiple_of(h * HEAD_SIZE, HEAD_SIZE), HEAD_SIZE)
            low = mixed[0:HEAD_SIZE].astype(jnp.bfloat16)
            part[where, kind, 0, rows, :] = low[:, 0:HALF]
            part[where, kind, 1, rows, :] = low[:, HALF:]
            tops[pl.ds(h, 1), :] = level
            sums[pl.ds(h, 1), :] = mixed[HEAD_SIZE : HEAD_SIZE + 1]
            return carry

        lax.fori_loop(0, GROUP_WIDTH, head, 0)
        for half in range(2):
            lanes = pl.ds(half * HALF, HALF)
            put_stats(part.at[where, kind, half], tops[:, lanes], sums[:, lanes])

    def put_stats(ref, top, total):
        high = total.astype(jnp.bfloat16).astype(jnp.float32)
        stats = jnp.concatenate([top, high, total - high, jnp.zeros_like(top)], axis=0)
        ref[OUT_ROWS:PART_ROWS, :] = stats.astype(jnp.bfloat16)

    def get_stats(ref):
        stats = ref[OUT_ROWS:PART_ROWS, :].astype(jnp.float32)
        return stats[0:8], stats[8:16] + stats[16:24]

    def merge(ref, others):
        pairs = [get_stats(r) for r in [ref] + others]
        top = functools.reduce(jnp.maximum, [p[0] for p in pairs])
        factors = [jnp.exp2(p[0] - top) for p in pairs]
        total = sum(p[1] * f for p, f in zip(pairs, factors))
        for h in range(GROUP_WIDTH):
            rows = slice(h * HEAD_SIZE, (h + 1) * HEAD_SIZE)
            acc = sum(
                r[rows, :].astype(jnp.float32) * f[h : h + 1]
                for r, f in zip([ref] + others, factors)
            )
            ref[rows, :] = acc.astype(jnp.bfloat16)
        put_stats(ref, top, total)

    halves = (0, 1)
    for half in halves:
        for direction in (0, 1):
            q_copy(direction, 1, half).start()
        q_core_copy(0, half).start()
    fetch_pool.wait()
    fetch_suffix.wait()
    attend(0, 0, True)
    pending = []

    def arrived(step, direction, half):
        q_copy(direction, step, half).wait_recv()
        if step + 1 < far or (step + 1 == far and half == direction):
            q_copy(direction, step + 1, half).start()
        q_core_copy(-step if direction == 0 else step, half).start()

    def other_core(offset):
        for half in halves:
            q_core_copy(offset, half).wait_recv()
        attend(offset, 1, False)
        p_core_copy(offset).start()

    for step in range(1, far):
        for direction in (0, 1):
            arrived(step, direction, 0)
        if step == 1:
            other_core(0)
        else:
            other_core(1 - step)
            other_core(step - 1)
        for direction in (0, 1):
            arrived(step, direction, 1)
        attend(-step, 0, False)
        attend(step, 0, False)
    arrived(far, 0, 0)
    arrived(far, 1, 1)
    attend(far, 0, False)
    other_core(far)
    other_core(1 - far)
    other_core(far - 1)

    p_core_copy(far).wait_recv()
    for direction in (0, 1):
        half = direction
        merge(part.at[far, 0, half], [partner_part.at[far, half]])
        p_copy(direction, far, half).start()
    for distance in range(far - 1, 0, -1):
        for direction in (0, 1):
            offset = (distance if direction == 0 else -distance) % chips
            p_core_copy(offset).wait_recv()
        for turn in (0, 1):
            for direction in (0, 1):
                offset = (distance if direction == 0 else -distance) % chips
                half = direction if turn == 1 else 1 - direction
                others = [partner_part.at[offset, half]]
                if distance < far - 1 or half == direction:
                    p_copy(direction, distance + 1, half).wait_recv()
                    others.append(ring_in.at[direction, distance, half])
                merge(part.at[offset, 0, half], others)
                p_copy(direction, distance, half).start()
    p_core_copy(0).wait_recv()
    for half in halves:
        for direction in (0, 1):
            p_copy(direction, 1, half).wait_recv()
        refs = [part.at[0, 0, half], partner_part.at[0, half], ring_in.at[0, 0, half], ring_in.at[1, 0, half]]
        pairs = [get_stats(r) for r in refs]
        top = functools.reduce(jnp.maximum, [p[0] for p in pairs])
        factors = [jnp.exp2(p[0] - top) for p in pairs]
        total = sum(p[1] * f for p, f in zip(pairs, factors))
        factors = [f / total for f in factors]
        for h in range(GROUP_WIDTH):
            rows = slice(h * HEAD_SIZE, (h + 1) * HEAD_SIZE)
            acc = sum(r[rows, :].astype(jnp.float32) * f[h : h + 1] for r, f in zip(refs, factors))
            out[half * HALF : (half + 1) * HALF, rows] = acc.T.astype(jnp.bfloat16)

    for direction in (0, 1):
        for half in halves:
            for step in range(1, far + 1):
                if step < far or half == direction:
                    q_copy(direction, step, half).wait_send()
                    p_copy(direction, step, half).wait_send()
    for offset in range(chips):
        for half in halves:
            q_core_copy(offset, half).wait_send()
        p_core_copy(offset).wait_send()


def attention(table, live, queries, kv_pages, suffix_key_value):
    chips = lax.axis_size("cache_0")
    capacity = table.shape[1]
    far = chips // 2
    long = capacity * PAGE_TOKENS + SUF
    bf16 = jnp.bfloat16
    requests = table.shape[0]
    any_space = pl.BlockSpec(memory_space=pl.ANY)
    flops = 4 * requests * GROUP_WIDTH * SUF * HEAD_SIZE * capacity * PAGE_TOKENS
    dma = pltpu.SemaphoreType.DMA
    return pl.pallas_call(
        functools.partial(attention_kernel, capacity, chips),
        out_shape=jax.ShapeDtypeStruct(queries.shape, bf16),
        in_specs=[
            pl.BlockSpec(memory_space=pltpu.SMEM),
            pl.BlockSpec(memory_space=pltpu.SMEM),
            any_space,
            any_space,
            any_space,
        ],
        out_specs=pl.BlockSpec(memory_space=pltpu.VMEM),
        scratch_shapes=[
            pltpu.VMEM(kv_pages.shape, bf16),
            pltpu.VMEM(suffix_key_value.shape, bf16),
            pltpu.VMEM((chips, 2) + queries.shape, bf16),
            pltpu.VMEM((chips, 2, 2, PART_ROWS, HALF), bf16),
            pltpu.VMEM((chips, 2, PART_ROWS, HALF), bf16),
            pltpu.VMEM((2, far, 2, PART_ROWS, HALF), bf16),
            pltpu.VMEM((long, HEAD_SIZE), bf16),
            pltpu.VMEM((VALUE_ROWS, long), bf16),
            pltpu.VMEM((long, SUF), jnp.float32),
            pltpu.VMEM((long, SUF), bf16),
            pltpu.VMEM((GROUP_WIDTH, SUF), jnp.float32),
            pltpu.VMEM((GROUP_WIDTH, SUF), jnp.float32),
            dma((3,)),
            dma((2, far, 2)),
            dma((2, far, 2)),
            dma((chips, 2)),
            dma((chips, 2)),
            dma((chips,)),
            dma((chips,)),
            dma((2, far, 2)),
            dma((2, far, 2)),
        ],
        compiler_params=pltpu.CompilerParams(
            collective_id=0, has_side_effects=True, vmem_limit_bytes=60 * 1024 * 1024
        ),
        cost_estimate=pl.CostEstimate(
            flops=8 * flops, bytes_accessed=kv_pages.size * 2, transcendentals=0
        ),
        name="ring_attention",
    )(table, live, queries, kv_pages, suffix_key_value)


def slot_tables(kv_pages, page_ids, prefix_pages, page_home):
    cache_count = lax.axis_size(CACHE)
    request_count = page_ids.shape[0]
    capacity = (3 * request_count * MAXP + 2 * cache_count - 1) // (2 * cache_count)
    pool_rows = kv_pages.shape[0]
    table_index = jnp.arange(page_home.shape[0], dtype=jnp.int32)
    owner_index = jnp.arange(cache_count, dtype=jnp.int32)
    buffer_index = jnp.arange(cache_count * capacity, dtype=jnp.int32)
    flat_ids = page_ids.reshape(-1)
    rows_of = jnp.sum(
        jnp.where(flat_ids[:, None] == table_index[None, :], page_home[None, :], 0), axis=1
    )
    owners = rows_of // pool_rows
    within = rows_of % pool_rows
    live_slots = (jnp.arange(MAXP, dtype=jnp.int32)[None, :] < prefix_pages[:, None]).reshape(-1)
    member = ((owners[:, None] == owner_index[None, :]) & live_slots[:, None]).astype(jnp.int32)
    earlier = jnp.cumsum(member, axis=0) - member
    rank_within = jnp.sum(earlier * member, axis=1)
    target = jnp.where(live_slots, owners * capacity + rank_within, -1)
    wanted = jnp.sum(
        jnp.where(target[:, None] == buffer_index[None, :], within[:, None] + 1, 0), axis=0
    )
    everyone = lax.all_gather(wanted, CACHE).reshape(cache_count, cache_count, capacity)
    mine = lax.dynamic_index_in_dim(everyone, lax.axis_index(CACHE), 1, keepdims=False)
    return jnp.maximum(mine - 1, 0), (mine > 0).astype(jnp.float32)


def per_device(queries, suffix_key_value, kv_pages, page_ids, prefix_pages, page_home, out_weight):
    table, live = slot_tables(kv_pages, page_ids, prefix_pages, page_home)
    outputs = attention(table, live, queries, kv_pages, suffix_key_value)

    def project(weight_piece, start_column):
        return jnp.dot(outputs, weight_piece, preferred_element_type=jnp.float32)

    group_term = on_gathered_pieces(out_weight, CACHE, 1, project, 1)
    attended = lax.psum_scatter(
        group_term.astype(jnp.bfloat16), "tensor", scatter_dimension=1, tiled=True
    )
    return attended


def solution(mesh):
    cores = 2
    chips = mesh.shape["cache"] // cores
    split = Mesh(
        mesh.devices.reshape(mesh.shape["groups"], chips, cores, mesh.shape["tensor"]),
        ("groups", "cache_0", "cache_1", "tensor"),
    )
    placed = (
        P(GROUPS_CACHE, "tensor"),
        P(None, GROUPS_CACHE, "tensor"),
        P(GROUPS_CACHE, None, None, "tensor"),
        P(GROUPS_CACHE, None),
        P(GROUPS_CACHE),
        P("groups"),
        P("tensor", CACHE),
    )
    return jax.shard_map(
        per_device,
        mesh=split,
        in_specs=placed,
        out_specs=P(GROUPS_CACHE, "tensor"),
        check_vma=False,
    )
```

```python
import functools

import jax
import jax.numpy as jnp
from jax import lax
from jax.experimental import pallas as pl
from jax.experimental.pallas import tpu as pltpu
from jax.sharding import Mesh
from jax.sharding import PartitionSpec as P

QUERY_HEADS = 64
KEY_VALUE_HEADS = 8
HEAD_SIZE = 128
PAGE_TOKENS = 128
SUF = 256
MAXP = 64
CACHE = ("cache_0", "cache_1")
GROUPS_CACHE = ("groups", "cache_0", "cache_1")
GROUP_WIDTH = QUERY_HEADS // KEY_VALUE_HEADS

LOG2_SCALE = HEAD_SIZE ** (-0.5) * 1.4426950408889634
DEAD = 1e30
HALF = SUF // 2
OUT_ROWS = GROUP_WIDTH * HEAD_SIZE
PART_ROWS = OUT_ROWS + 32
VALUE_ROWS = HEAD_SIZE + 16
MESH = pl.DeviceIdType.MESH


def prefill_kernel(
    capacity,
    chips,
    spans,
    own_table,
    table_hbm,
    q_hbm,
    kv_hbm,
    suffix_hbm,
    weight_hbm,
    out_hbm,
    pool,
    suffix,
    weight,
    q_all,
    part,
    partner_part,
    ring_in,
    keys,
    values_t,
    scores,
    weights,
    tops,
    sums,
    tables,
    tables_in,
    mixed_all,
    terms,
    terms_in,
    finished,
    landed,
    local_sem,
    table_send,
    table_recv,
    q_send,
    q_recv,
    q_core_send,
    q_core_recv,
    p_core_send,
    p_core_recv,
    p_send,
    p_recv,
    m_send,
    m_recv,
    m_core_send,
    m_core_recv,
    t_send,
    t_recv,
    f_send,
    f_recv,
):
    x = lax.axis_index("cache_0")
    core = lax.axis_index("cache_1")
    y = lax.axis_index("tensor")
    me = 2 * x + core
    caches = 2 * chips
    slabs = caches // spans
    goal = me // slabs
    at_goal = goal == y
    right = {"cache_0": lax.rem(x + 1, chips), "cache_1": core}
    left = {"cache_0": lax.rem(x + chips - 1, chips), "cache_1": core}
    partner = {"cache_0": x, "cache_1": 1 - core}
    up = {"tensor": lax.rem(y + 1, spans)}
    down = {"tensor": lax.rem(y + spans - 1, spans)}
    far = chips // 2
    far_span = spans // 2
    toward = (right, left)
    toward_span = (up, down)
    peers = [(dx, dk) for dx in range(chips) for dk in (0, 1)]

    def cache_peer(dx, dk):
        return {"cache_0": lax.rem(x + dx, chips), "cache_1": core if dk == 0 else 1 - core}

    def source_peer(dj, dv):
        cache = y * slabs + lax.rem(me + dj, slabs)
        return {"cache_0": cache // 2, "cache_1": lax.rem(cache, 2), "tensor": lax.rem(y + dv, spans)}

    fetch_q = pltpu.make_async_copy(q_hbm, q_all.at[0, 0], local_sem.at[0])
    fetch_table = pltpu.make_async_copy(table_hbm, tables_in.at[0], local_sem.at[1])
    fetch_pool = pltpu.make_async_copy(kv_hbm, pool, local_sem.at[2])
    fetch_suffix = pltpu.make_async_copy(suffix_hbm, suffix, local_sem.at[3])
    fetch_weight = pltpu.make_async_copy(weight_hbm, weight, local_sem.at[4])
    fetch_q.start()
    fetch_table.start()
    fetch_pool.start()
    fetch_suffix.start()
    fetch_weight.start()
    barrier = pltpu.get_barrier_semaphore()
    for dx, dk in peers[1:]:
        pl.semaphore_signal(barrier, inc=1, device_id=cache_peer(dx, dk), device_id_type=MESH)
    for peer in toward_span:
        pl.semaphore_signal(barrier, inc=1, device_id=peer, device_id_type=MESH)
    for dj in range(slabs):
        for dv in range(spans):
            pl.semaphore_signal(barrier, inc=1, device_id=source_peer(dj, dv), device_id_type=MESH)
    values_t[HEAD_SIZE:, :] = jnp.ones((VALUE_ROWS - HEAD_SIZE, values_t.shape[1]), jnp.bfloat16)
    fetch_q.wait()
    fetch_table.wait()
    pl.semaphore_wait(barrier, caches - 1 + 2 + caches)

    def chunk(offset, kind, half):
        return q_all.at[offset % chips, kind, pl.ds(half * HALF, HALF), :]

    def q_copy(direction, step, half):
        sign = -1 if direction == 0 else 1
        return pltpu.make_async_remote_copy(
            src_ref=chunk(sign * (step - 1), 0, half),
            dst_ref=chunk(sign * step, 0, half),
            send_sem=q_send.at[direction, step - 1, half],
            recv_sem=q_recv.at[direction, step - 1, half],
            device_id=toward[direction],
            device_id_type=MESH,
        )

    def q_core_copy(offset, half):
        return pltpu.make_async_remote_copy(
            src_ref=chunk(offset, 0, half),
            dst_ref=chunk(offset, 1, half),
            send_sem=q_core_send.at[offset % chips, half],
            recv_sem=q_core_recv.at[offset % chips, half],
            device_id=partner,
            device_id_type=MESH,
        )

    def p_core_copy(offset):
        return pltpu.make_async_remote_copy(
            src_ref=part.at[offset % chips, 1],
            dst_ref=partner_part.at[offset % chips],
            send_sem=p_core_send.at[offset % chips],
            recv_sem=p_core_recv.at[offset % chips],
            device_id=partner,
            device_id_type=MESH,
        )

    def table_copy(dx, dk):
        place = 2 * ((-dx) % chips) + dk
        return pltpu.make_async_remote_copy(
            src_ref=tables_in.at[0],
            dst_ref=tables_in.at[place],
            send_sem=table_send.at[place],
            recv_sem=table_recv.at[place],
            device_id=cache_peer(dx, dk),
            device_id_type=MESH,
        )

    def table_load(place):
        return pltpu.make_async_copy(tables_in.at[place], tables.at[place], local_sem.at[5])

    def p_copy(direction, distance, half):
        sign = 1 if direction == 0 else -1
        return pltpu.make_async_remote_copy(
            src_ref=part.at[(sign * distance) % chips, 0, half],
            dst_ref=ring_in.at[direction, distance - 1, half],
            send_sem=p_send.at[direction, distance - 1, half],
            recv_sem=p_recv.at[direction, distance - 1, half],
            device_id=toward[direction],
            device_id_type=MESH,
        )

    def attend(offset, kind, own):
        where = offset % chips
        place = 2 * where + kind
        pages = capacity + (SUF // PAGE_TOKENS if own else 0)
        alive = []
        for j in range(capacity):
            if own:
                entry = own_table[0, me * capacity + j]
            else:
                entry = tables[place, 0, me * capacity + j]
            row = jnp.maximum(entry - 1, 0)
            alive.append(jnp.minimum(entry, 1).astype(jnp.float32))
            keys[j * PAGE_TOKENS : (j + 1) * PAGE_TOKENS, :] = pool[row, 0]
            values_t[0:HEAD_SIZE, j * PAGE_TOKENS : (j + 1) * PAGE_TOKENS] = pool[row, 1].T
        if own:
            keys[capacity * PAGE_TOKENS :, :] = suffix[0]
            values_t[0:HEAD_SIZE, capacity * PAGE_TOKENS :] = suffix[1].T

        def head(h, carry):
            q_head = q_all[where, kind, :, pl.ds(pl.multiple_of(h * HEAD_SIZE, HEAD_SIZE), HEAD_SIZE)]
            top = None
            for j in range(pages):
                span = pl.ds(j * PAGE_TOKENS, PAGE_TOKENS)
                piece = lax.dot_general(
                    keys[span, :], q_head, (((1,), (1,)), ((), ())), preferred_element_type=jnp.float32
                )
                if j >= capacity:
                    key_at = lax.broadcasted_iota(jnp.int32, piece.shape, 0) + (j - capacity) * PAGE_TOKENS
                    token_at = lax.broadcasted_iota(jnp.int32, piece.shape, 1)
                    piece = jnp.where(key_at <= token_at, piece, -DEAD)
                scores[span, :] = piece
                peak = jnp.max(piece, axis=0, keepdims=True)
                if j < capacity:
                    peak = peak * alive[j] + (alive[j] - 1.0) * DEAD
                top = peak if top is None else jnp.maximum(top, peak)
            level = jnp.ceil(top * (LOG2_SCALE * 0.25)) * 4.0
            for j in range(pages):
                span = pl.ds(j * PAGE_TOKENS, PAGE_TOKENS)
                shift = -level
                if j < capacity:
                    shift = shift * alive[j] + (alive[j] - 1.0) * DEAD
                weights[span, :] = jnp.exp2(scores[span, :] * LOG2_SCALE + shift).astype(jnp.bfloat16)
            length = pages * PAGE_TOKENS
            mixed = jnp.dot(values_t[:, 0:length], weights[0:length, :], preferred_element_type=jnp.float32)
            rows = pl.ds(pl.multiple_of(h * HEAD_SIZE, HEAD_SIZE), HEAD_SIZE)
            low = mixed[0:HEAD_SIZE].astype(jnp.bfloat16)
            part[where, kind, 0, rows, :] = low[:, 0:HALF]
            part[where, kind, 1, rows, :] = low[:, HALF:]
            tops[pl.ds(h, 1), :] = level
            sums[pl.ds(h, 1), :] = mixed[HEAD_SIZE : HEAD_SIZE + 1]
            return carry

        lax.fori_loop(0, GROUP_WIDTH, head, 0)
        for half in range(2):
            lanes = pl.ds(half * HALF, HALF)
            put_stats(part.at[where, kind, half], tops[:, lanes], sums[:, lanes])

    def put_stats(ref, top, total):
        high = total.astype(jnp.bfloat16).astype(jnp.float32)
        stats = jnp.concatenate([top, high, total - high, jnp.zeros_like(top)], axis=0)
        ref[OUT_ROWS:PART_ROWS, :] = stats.astype(jnp.bfloat16)

    def get_stats(ref):
        stats = ref[OUT_ROWS:PART_ROWS, :].astype(jnp.float32)
        return stats[0:8], stats[8:16] + stats[16:24]

    def merge(ref, others):
        pairs = [get_stats(r) for r in [ref] + others]
        top = functools.reduce(jnp.maximum, [p[0] for p in pairs])
        factors = [jnp.exp2(p[0] - top) for p in pairs]
        total = sum(p[1] * f for p, f in zip(pairs, factors))
        for h in range(GROUP_WIDTH):
            rows = slice(h * HEAD_SIZE, (h + 1) * HEAD_SIZE)
            acc = sum(
                r[rows, :].astype(jnp.float32) * f[h : h + 1]
                for r, f in zip([ref] + others, factors)
            )
            ref[rows, :] = acc.astype(jnp.bfloat16)
        put_stats(ref, top, total)

    halves = (0, 1)
    for half in halves:
        for direction in (0, 1):
            q_copy(direction, 1, half).start()
        q_core_copy(0, half).start()
    for dx, dk in peers[1:]:
        table_copy(dx, dk).start()
    fetch_pool.wait()
    fetch_suffix.wait()
    attend(0, 0, True)
    for dx, dk in peers[1:]:
        table_copy(dx, dk).wait_recv()
        place = 2 * ((-dx) % chips) + dk
        load = table_load(place)
        load.start()
        load.wait()

    def arrived(step, direction, half):
        q_copy(direction, step, half).wait_recv()
        if step + 1 < far or (step + 1 == far and half == direction):
            q_copy(direction, step + 1, half).start()
        q_core_copy(-step if direction == 0 else step, half).start()

    def other_core(offset):
        for half in halves:
            q_core_copy(offset, half).wait_recv()
        attend(offset, 1, False)
        p_core_copy(offset).start()

    for step in range(1, far):
        for direction in (0, 1):
            arrived(step, direction, 0)
        if step == 1:
            other_core(0)
        else:
            other_core(1 - step)
            other_core(step - 1)
        for direction in (0, 1):
            arrived(step, direction, 1)
        attend(-step, 0, False)
        attend(step, 0, False)
    arrived(far, 0, 0)
    arrived(far, 1, 1)
    attend(far, 0, False)
    other_core(far)
    other_core(1 - far)
    other_core(far - 1)

    p_core_copy(far).wait_recv()
    for direction in (0, 1):
        half = direction
        merge(part.at[far, 0, half], [partner_part.at[far, half]])
        p_copy(direction, far, half).start()
    for distance in range(far - 1, 0, -1):
        for direction in (0, 1):
            offset = (distance if direction == 0 else -distance) % chips
            p_core_copy(offset).wait_recv()
        for turn in (0, 1):
            for direction in (0, 1):
                offset = (distance if direction == 0 else -distance) % chips
                half = direction if turn == 1 else 1 - direction
                others = [partner_part.at[offset, half]]
                if distance < far - 1 or half == direction:
                    p_copy(direction, distance + 1, half).wait_recv()
                    others.append(ring_in.at[direction, distance, half])
                merge(part.at[offset, 0, half], others)
                p_copy(direction, distance, half).start()
    def mixed_chunk(offset, kind, half):
        return mixed_all.at[offset % chips, kind, pl.ds(half * HALF, HALF), :]

    def m_copy(direction, step, half):
        sign = -1 if direction == 0 else 1
        return pltpu.make_async_remote_copy(
            src_ref=mixed_chunk(sign * (step - 1), 0, half),
            dst_ref=mixed_chunk(sign * step, 0, half),
            send_sem=m_send.at[direction, step - 1, half],
            recv_sem=m_recv.at[direction, step - 1, half],
            device_id=toward[direction],
            device_id_type=MESH,
        )

    def m_core_copy(offset, half):
        return pltpu.make_async_remote_copy(
            src_ref=mixed_chunk(offset, 0, half),
            dst_ref=mixed_chunk(offset, 1, half),
            send_sem=m_core_send.at[offset % chips, half],
            recv_sem=m_core_recv.at[offset % chips, half],
            device_id=partner,
            device_id_type=MESH,
        )

    p_core_copy(0).wait_recv()
    for half in halves:
        for direction in (0, 1):
            p_copy(direction, 1, half).wait_recv()
        refs = [part.at[0, 0, half], partner_part.at[0, half], ring_in.at[0, 0, half], ring_in.at[1, 0, half]]
        pairs = [get_stats(r) for r in refs]
        top = functools.reduce(jnp.maximum, [p[0] for p in pairs])
        factors = [jnp.exp2(p[0] - top) for p in pairs]
        total = sum(p[1] * f for p, f in zip(pairs, factors))
        factors = [f / total for f in factors]
        for h in range(GROUP_WIDTH):
            rows = slice(h * HEAD_SIZE, (h + 1) * HEAD_SIZE)
            acc = sum(r[rows, :].astype(jnp.float32) * f[h : h + 1] for r, f in zip(refs, factors))
            mixed_all[0, 0, half * HALF : (half + 1) * HALF, rows] = acc.T.astype(jnp.bfloat16)
        for direction in (0, 1):
            if far > 1 or half == direction:
                m_copy(direction, 1, half).start()
        m_core_copy(0, half).start()
    fetch_weight.wait()

    def mixed_arrived(step, direction, half):
        m_copy(direction, step, half).wait_recv()
        if step + 1 < far or (step + 1 == far and half == direction):
            m_copy(direction, step + 1, half).start()
        m_core_copy(-step if direction == 0 else step, half).start()

    def t_copy(batch, direction, distance, half):
        index, first, count = batch
        sign = 1 if direction == 0 else -1
        return pltpu.make_async_remote_copy(
            src_ref=terms.at[(sign * distance) % spans, half, pl.ds(first, count)],
            dst_ref=terms_in.at[direction, distance - 1, half, pl.ds(first, count)],
            send_sem=t_send.at[index, direction, distance - 1, half],
            recv_sem=t_recv.at[index, direction, distance - 1, half],
            device_id=toward_span[direction],
            device_id_type=MESH,
        )

    block_rows = terms.shape[3]
    half_columns = terms.shape[4]
    place_rows = pl.ds(pl.multiple_of(y * block_rows, block_rows), block_rows)
    place_columns = pl.ds(pl.multiple_of(lax.rem(me, slabs) * 2 * half_columns, 2 * half_columns), 2 * half_columns)

    def f_copy(slot, offset, kind):
        target = dict(cache_peer(offset % chips, kind), tensor=goal)
        return pltpu.make_async_remote_copy(
            src_ref=finished.at[slot],
            dst_ref=landed.at[place_rows, place_columns],
            send_sem=f_send.at[slot],
            recv_sem=f_recv.at[y, lax.rem(me, slabs)],
            device_id=target,
            device_id_type=MESH,
        )

    def project(slot, offset, kind):
        term = jnp.dot(mixed_all[offset % chips, kind], weight[...], preferred_element_type=jnp.float32)
        low = term.astype(jnp.bfloat16)
        for block in range(spans):
            where = lax.rem(block - y + spans, spans)
            for half in halves:
                terms[where, half, slot] = low[
                    block * block_rows : (block + 1) * block_rows,
                    half * half_columns : (half + 1) * half_columns,
                ]

    def reduce_terms(batch, members):
        index, first, count = batch
        here = pl.ds(first, count)

        def passed_on(direction, distance, half):
            where = (distance if direction == 0 else -distance) % spans
            if distance < far_span - 1 or half == direction:
                t_copy(batch, direction, distance + 1, half).wait_recv()
                terms[where, half, here] = (
                    terms[where, half, here].astype(jnp.float32)
                    + terms_in[direction, distance, half, here].astype(jnp.float32)
                ).astype(jnp.bfloat16)
            t_copy(batch, direction, distance, half).start()

        def finish(half):
            for direction in (0, 1):
                if far_span > 1 or half == direction:
                    t_copy(batch, direction, 1, half).wait_recv()
            total = terms[0, half, here].astype(jnp.float32)
            for direction in (0, 1):
                if far_span > 1 or half == direction:
                    total = total + terms_in[direction, 0, half, here].astype(jnp.float32)
            finished[here, :, half * half_columns : (half + 1) * half_columns] = total.astype(jnp.bfloat16)

        for direction in (0, 1):
            t_copy(batch, direction, far_span, direction).start()
        if far_span > 1:
            for direction in (0, 1):
                passed_on(direction, far_span - 1, 1 - direction)
        yield
        for distance in range(far_span - 1, 0, -1):
            for direction in (0, 1):
                passed_on(direction, distance, direction)
            if distance > 1:
                for direction in (0, 1):
                    passed_on(direction, distance - 1, 1 - direction)
            yield
        for half in halves:
            finish(half)
        for slot, (offset, kind) in enumerate(members, first):
            if offset == 0 and kind == 0:

                @pl.when(at_goal)
                def _():
                    landed[place_rows, place_columns] = finished[slot]

                @pl.when(jnp.logical_not(at_goal))
                def _():
                    f_copy(slot, offset, kind).start()

            else:
                f_copy(slot, offset, kind).start()

    batches = [[(0, 0), (0, 1)]]
    for step in range(1, far):
        batches.append([(-step, 0), (step, 0), (-step, 1), (step, 1)])
    batches.append([(far, 0), (far, 1)])
    active = []

    def launch(index):
        first = sum(len(b) for b in batches[:index])
        for slot, (offset, kind) in enumerate(batches[index], first):
            if kind == 1:
                for half in halves:
                    m_core_copy(offset, half).wait_recv()
            project(slot, offset, kind)
        active.append(reduce_terms((index, first, len(batches[index])), batches[index]))
        next(active[-1])

    def advance():
        for item in list(active):
            try:
                next(item)
            except StopIteration:
                active.remove(item)

    for step in range(1, far):
        for direction in (0, 1):
            mixed_arrived(step, direction, 0)
        advance()
        launch(step - 1)
        for direction in (0, 1):
            mixed_arrived(step, direction, 1)
        advance()
    mixed_arrived(far, 0, 0)
    mixed_arrived(far, 1, 1)
    advance()
    launch(far - 1)
    advance()
    launch(far)
    while active:
        advance()

    for dj in range(slabs):
        for dv in range(spans):

            def take():
                block = lax.rem(y + dv, spans)
                slab = lax.rem(me + dj, slabs)
                pltpu.make_async_remote_copy(
                    src_ref=finished.at[0],
                    dst_ref=landed.at[place_rows, place_columns],
                    send_sem=f_send.at[0],
                    recv_sem=f_recv.at[block, slab],
                    device_id=partner,
                    device_id_type=MESH,
                ).wait_recv()

            if dj == 0 and dv == 0:
                pl.when(jnp.logical_not(at_goal))(take)
            else:
                take()
    store = pltpu.make_async_copy(landed, out_hbm, local_sem.at[6])
    store.start()

    for direction in (0, 1):
        for half in halves:
            for step in range(1, far + 1):
                if step < far or half == direction:
                    q_copy(direction, step, half).wait_send()
                    p_copy(direction, step, half).wait_send()
                    m_copy(direction, step, half).wait_send()
            for step in range(1, far_span + 1):
                if step < far_span or half == direction:
                    first = 0
                    for index, members in enumerate(batches):
                        t_copy((index, first, len(members)), direction, step, half).wait_send()
                        first += len(members)
    for offset in range(chips):
        for half in halves:
            q_core_copy(offset, half).wait_send()
            m_core_copy(offset, half).wait_send()
        p_core_copy(offset).wait_send()
    for dx, dk in peers[1:]:
        table_copy(dx, dk).wait_send()
    slot = 0
    for members in batches:
        for offset, kind in members:
            if slot == 0:

                @pl.when(jnp.logical_not(at_goal))
                def _():
                    f_copy(0, 0, 0).wait_send()

            else:
                f_copy(slot, offset, kind).wait_send()
            slot += 1
    store.wait()


def prefill(table, queries, kv_pages, suffix_key_value, out_weight):
    chips = lax.axis_size("cache_0")
    spans = lax.axis_size("tensor")
    caches = 2 * chips
    capacity = (3 * MAXP + 2 * caches - 1) // (2 * caches)
    far = chips // 2
    far_span = spans // 2
    long = capacity * PAGE_TOKENS + SUF
    width = out_weight.shape[1]
    bf16 = jnp.bfloat16
    any_space = pl.BlockSpec(memory_space=pl.ANY)
    flops = 4 * caches * GROUP_WIDTH * SUF * HEAD_SIZE * capacity * PAGE_TOKENS
    dma = pltpu.SemaphoreType.DMA
    out_shape = (SUF, width * caches // spans)
    return pl.pallas_call(
        functools.partial(prefill_kernel, capacity, chips, spans),
        out_shape=jax.ShapeDtypeStruct(out_shape, bf16),
        in_specs=[pl.BlockSpec(memory_space=pltpu.SMEM)] + [any_space] * 5,
        out_specs=any_space,
        scratch_shapes=[
            pltpu.VMEM(kv_pages.shape, bf16),
            pltpu.VMEM(suffix_key_value.shape, bf16),
            pltpu.VMEM(out_weight.shape, bf16),
            pltpu.VMEM((chips, 2) + queries.shape, bf16),
            pltpu.VMEM((chips, 2, 2, PART_ROWS, HALF), bf16),
            pltpu.VMEM((chips, 2, PART_ROWS, HALF), bf16),
            pltpu.VMEM((2, far, 2, PART_ROWS, HALF), bf16),
            pltpu.VMEM((long, HEAD_SIZE), bf16),
            pltpu.VMEM((VALUE_ROWS, long), bf16),
            pltpu.VMEM((long, SUF), jnp.float32),
            pltpu.VMEM((long, SUF), bf16),
            pltpu.VMEM((GROUP_WIDTH, SUF), jnp.float32),
            pltpu.VMEM((GROUP_WIDTH, SUF), jnp.float32),
            pltpu.SMEM((caches,) + table.shape, jnp.int32),
            pltpu.VMEM((caches,) + table.shape, jnp.int32),
            pltpu.VMEM((chips, 2) + queries.shape, bf16),
            pltpu.VMEM((spans, 2, caches, SUF // spans, width // 2), bf16),
            pltpu.VMEM((2, far_span, 2, caches, SUF // spans, width // 2), bf16),
            pltpu.VMEM((caches, SUF // spans, width), bf16),
            pltpu.VMEM(out_shape, bf16),
            dma((7,)),
            dma((caches,)),
            dma((caches,)),
            dma((2, far, 2)),
            dma((2, far, 2)),
            dma((chips, 2)),
            dma((chips, 2)),
            dma((chips,)),
            dma((chips,)),
            dma((2, far, 2)),
            dma((2, far, 2)),
            dma((2, far, 2)),
            dma((2, far, 2)),
            dma((chips, 2)),
            dma((chips, 2)),
            dma((far + 1, 2, far_span, 2)),
            dma((far + 1, 2, far_span, 2)),
            dma((caches,)),
            dma((spans, caches // spans)),
        ],
        compiler_params=pltpu.CompilerParams(
            collective_id=0, has_side_effects=True, vmem_limit_bytes=62 * 1024 * 1024
        ),
        cost_estimate=pl.CostEstimate(
            flops=flops, bytes_accessed=kv_pages.size * 2, transcendentals=0
        ),
        name="prefill",
    )(table, table, queries, kv_pages, suffix_key_value, out_weight)


def slot_tables(kv_pages, page_ids, prefix_pages, page_home):
    cache_count = lax.axis_size(CACHE)
    request_count = page_ids.shape[0]
    capacity = (3 * request_count * MAXP + 2 * cache_count - 1) // (2 * cache_count)
    pool_rows = kv_pages.shape[0]
    table_index = jnp.arange(page_home.shape[0], dtype=jnp.int32)
    owner_index = jnp.arange(cache_count, dtype=jnp.int32)
    buffer_index = jnp.arange(cache_count * capacity, dtype=jnp.int32)
    flat_ids = page_ids.reshape(-1)
    rows_of = jnp.sum(
        jnp.where(flat_ids[:, None] == table_index[None, :], page_home[None, :], 0), axis=1
    )
    owners = rows_of // pool_rows
    within = rows_of % pool_rows
    live_slots = (jnp.arange(MAXP, dtype=jnp.int32)[None, :] < prefix_pages[:, None]).reshape(-1)
    member = ((owners[:, None] == owner_index[None, :]) & live_slots[:, None]).astype(jnp.int32)
    earlier = jnp.cumsum(member, axis=0) - member
    rank_within = jnp.sum(earlier * member, axis=1)
    target = jnp.where(live_slots, owners * capacity + rank_within, -1)
    wanted = jnp.sum(
        jnp.where(target[:, None] == buffer_index[None, :], within[:, None] + 1, 0), axis=0
    )
    lanes = 128 * ((wanted.shape[0] + 127) // 128)
    return jnp.pad(wanted, (0, lanes - wanted.shape[0]))[None, :]


def per_device(queries, suffix_key_value, kv_pages, page_ids, prefix_pages, page_home, out_weight):
    table = slot_tables(kv_pages, page_ids, prefix_pages, page_home)
    return prefill(table, queries, kv_pages, suffix_key_value, out_weight)


def solution(mesh):
    cores = 2
    chips = mesh.shape["cache"] // cores
    split = Mesh(
        mesh.devices.reshape(mesh.shape["groups"], chips, cores, mesh.shape["tensor"]),
        ("groups", "cache_0", "cache_1", "tensor"),
    )
    placed = (
        P(GROUPS_CACHE, "tensor"),
        P(None, GROUPS_CACHE, "tensor"),
        P(GROUPS_CACHE, None, None, "tensor"),
        P(GROUPS_CACHE, None),
        P(GROUPS_CACHE),
        P("groups"),
        P("tensor", CACHE),
    )
    return jax.shard_map(
        per_device,
        mesh=split,
        in_specs=placed,
        out_specs=P(GROUPS_CACHE, "tensor"),
        check_vma=False,
    )
```

```python
import functools

import jax
import jax.numpy as jnp
from jax import lax
from jax.experimental import pallas as pl
from jax.experimental.pallas import tpu as pltpu
from jax.sharding import Mesh
from jax.sharding import PartitionSpec as P

QUERY_HEADS = 64
KEY_VALUE_HEADS = 8
HEAD_SIZE = 128
PAGE_TOKENS = 128
SUF = 256
MAXP = 64
CACHE = ("cache_0", "cache_1")
GROUPS_CACHE = ("groups", "cache_0", "cache_1")
GROUP_WIDTH = QUERY_HEADS // KEY_VALUE_HEADS

LOG2_SCALE = HEAD_SIZE ** (-0.5) * 1.4426950408889634
DEAD = 1e30
HALF = SUF // 2
OUT_ROWS = GROUP_WIDTH * HEAD_SIZE
PART_ROWS = OUT_ROWS + 32
VALUE_ROWS = HEAD_SIZE + 16
MESH = pl.DeviceIdType.MESH


def prefill_kernel(
    capacity,
    chips,
    spans,
    own_table,
    table_hbm,
    q_hbm,
    kv_hbm,
    suffix_hbm,
    weight_hbm,
    out_hbm,
    pool,
    suffix,
    weight,
    q_all,
    part,
    partner_part,
    ring_in,
    keys,
    values_t,
    scores,
    weights,
    tops,
    sums,
    tables,
    tables_in,
    mixed_all,
    terms,
    terms_in,
    finished,
    landed,
    local_sem,
    table_send,
    table_recv,
    q_send,
    q_recv,
    q_core_send,
    q_core_recv,
    p_core_send,
    p_core_recv,
    p_send,
    p_recv,
    m_send,
    m_recv,
    m_core_send,
    m_core_recv,
    t_send,
    t_recv,
    f_send,
    f_recv,
):
    x = lax.axis_index("cache_0")
    core = lax.axis_index("cache_1")
    y = lax.axis_index("tensor")
    me = 2 * x + core
    caches = 2 * chips
    slabs = caches // spans
    goal = me // slabs
    at_goal = goal == y
    right = {"cache_0": lax.rem(x + 1, chips), "cache_1": core}
    left = {"cache_0": lax.rem(x + chips - 1, chips), "cache_1": core}
    partner = {"cache_0": x, "cache_1": 1 - core}
    up = {"tensor": lax.rem(y + 1, spans)}
    down = {"tensor": lax.rem(y + spans - 1, spans)}
    far = chips // 2
    far_span = spans // 2
    toward = (right, left)
    toward_span = (up, down)
    peers = [(dx, dk) for dx in range(chips) for dk in (0, 1)]

    def cache_peer(dx, dk):
        return {"cache_0": lax.rem(x + dx, chips), "cache_1": core if dk == 0 else 1 - core}

    def source_peer(dj, dv):
        cache = y * slabs + lax.rem(me + dj, slabs)
        return {"cache_0": cache // 2, "cache_1": lax.rem(cache, 2), "tensor": lax.rem(y + dv, spans)}

    fetch_q = pltpu.make_async_copy(q_hbm, q_all.at[0, 0], local_sem.at[0])
    fetch_table = pltpu.make_async_copy(table_hbm, tables_in.at[0], local_sem.at[1])
    fetch_pool = pltpu.make_async_copy(kv_hbm, pool, local_sem.at[2])
    fetch_suffix = pltpu.make_async_copy(suffix_hbm, suffix, local_sem.at[3])
    fetch_weight = pltpu.make_async_copy(weight_hbm, weight, local_sem.at[4])
    fetch_q.start()
    fetch_table.start()
    fetch_pool.start()
    fetch_suffix.start()
    fetch_weight.start()
    barrier = pltpu.get_barrier_semaphore()
    for dx, dk in peers[1:]:
        pl.semaphore_signal(barrier, inc=1, device_id=cache_peer(dx, dk), device_id_type=MESH)
    for peer in toward_span:
        pl.semaphore_signal(barrier, inc=1, device_id=peer, device_id_type=MESH)
    for dj in range(slabs):
        for dv in range(spans):
            pl.semaphore_signal(barrier, inc=1, device_id=source_peer(dj, dv), device_id_type=MESH)
    values_t[HEAD_SIZE:, :] = jnp.ones((VALUE_ROWS - HEAD_SIZE, values_t.shape[1]), jnp.bfloat16)
    fetch_q.wait()
    fetch_table.wait()
    pl.semaphore_wait(barrier, caches - 1 + 2 + caches)

    def chunk(offset, kind, half):
        return q_all.at[offset % chips, kind, pl.ds(half * HALF, HALF), :]

    def q_copy(direction, step, half):
        sign = -1 if direction == 0 else 1
        return pltpu.make_async_remote_copy(
            src_ref=chunk(sign * (step - 1), 0, half),
            dst_ref=chunk(sign * step, 0, half),
            send_sem=q_send.at[direction, step - 1, half],
            recv_sem=q_recv.at[direction, step - 1, half],
            device_id=toward[direction],
            device_id_type=MESH,
        )

    def q_core_copy(offset, half):
        return pltpu.make_async_remote_copy(
            src_ref=chunk(offset, 0, half),
            dst_ref=chunk(offset, 1, half),
            send_sem=q_core_send.at[offset % chips, half],
            recv_sem=q_core_recv.at[offset % chips, half],
            device_id=partner,
            device_id_type=MESH,
        )

    def p_core_copy(offset):
        return pltpu.make_async_remote_copy(
            src_ref=part.at[offset % chips, 1],
            dst_ref=partner_part.at[offset % chips],
            send_sem=p_core_send.at[offset % chips],
            recv_sem=p_core_recv.at[offset % chips],
            device_id=partner,
            device_id_type=MESH,
        )

    def table_copy(dx, dk):
        place = 2 * ((-dx) % chips) + dk
        return pltpu.make_async_remote_copy(
            src_ref=tables_in.at[0],
            dst_ref=tables_in.at[place],
            send_sem=table_send.at[place],
            recv_sem=table_recv.at[place],
            device_id=cache_peer(dx, dk),
            device_id_type=MESH,
        )

    def table_load(place):
        return pltpu.make_async_copy(tables_in.at[place], tables.at[place], local_sem.at[5])

    def p_copy(direction, distance, half):
        sign = 1 if direction == 0 else -1
        return pltpu.make_async_remote_copy(
            src_ref=part.at[(sign * distance) % chips, 0, half],
            dst_ref=ring_in.at[direction, distance - 1, half],
            send_sem=p_send.at[direction, distance - 1, half],
            recv_sem=p_recv.at[direction, distance - 1, half],
            device_id=toward[direction],
            device_id_type=MESH,
        )

    def attend(offset, kind, own):
        where = offset % chips
        place = 2 * where + kind
        pages = capacity + (SUF // PAGE_TOKENS if own else 0)
        alive = []
        for j in range(capacity):
            if own:
                entry = own_table[0, me * capacity + j]
            else:
                entry = tables[place, 0, me * capacity + j]
            row = jnp.maximum(entry - 1, 0)
            alive.append(jnp.minimum(entry, 1).astype(jnp.float32))
            keys[j * PAGE_TOKENS : (j + 1) * PAGE_TOKENS, :] = pool[row, 0]
            values_t[0:HEAD_SIZE, j * PAGE_TOKENS : (j + 1) * PAGE_TOKENS] = pool[row, 1].T
        if own:
            keys[capacity * PAGE_TOKENS :, :] = suffix[0]
            values_t[0:HEAD_SIZE, capacity * PAGE_TOKENS :] = suffix[1].T

        length = pages * PAGE_TOKENS

        def score(h, slot):
            q_head = q_all[where, kind, :, pl.ds(pl.multiple_of(h * HEAD_SIZE, HEAD_SIZE), HEAD_SIZE)]
            top = None
            for j in range(pages):
                span = pl.ds(j * PAGE_TOKENS, PAGE_TOKENS)
                piece = lax.dot_general(
                    keys[span, :], q_head, (((1,), (1,)), ((), ())), preferred_element_type=jnp.float32
                )
                if j >= capacity:
                    key_at = lax.broadcasted_iota(jnp.int32, piece.shape, 0) + (j - capacity) * PAGE_TOKENS
                    token_at = lax.broadcasted_iota(jnp.int32, piece.shape, 1)
                    piece = jnp.where(key_at <= token_at, piece, -DEAD)
                scores[slot, span, :] = piece
                peak = jnp.max(piece, axis=0, keepdims=True)
                if j < capacity:
                    peak = peak * alive[j] + (alive[j] - 1.0) * DEAD
                top = peak if top is None else jnp.maximum(top, peak)
            return jnp.ceil(top * (LOG2_SCALE * 0.25)) * 4.0

        def gather_values(h, slot, level):
            for j in range(pages):
                span = pl.ds(j * PAGE_TOKENS, PAGE_TOKENS)
                shift = -level
                if j < capacity:
                    shift = shift * alive[j] + (alive[j] - 1.0) * DEAD
                weights[slot, span, :] = jnp.exp2(scores[slot, span, :] * LOG2_SCALE + shift).astype(jnp.bfloat16)
            mixed = jnp.dot(values_t[:, 0:length], weights[slot, 0:length, :], preferred_element_type=jnp.float32)
            rows = pl.ds(pl.multiple_of(h * HEAD_SIZE, HEAD_SIZE), HEAD_SIZE)
            low = mixed[0:HEAD_SIZE].astype(jnp.bfloat16)
            part[where, kind, 0, rows, :] = low[:, 0:HALF]
            part[where, kind, 1, rows, :] = low[:, HALF:]
            tops[pl.ds(h, 1), :] = level
            sums[pl.ds(h, 1), :] = mixed[HEAD_SIZE : HEAD_SIZE + 1]

        def two_heads(i, level):
            later = score(2 * i + 1, 1)
            gather_values(2 * i, 0, level)
            following = score(jnp.minimum(2 * i + 2, GROUP_WIDTH - 1), 0)
            gather_values(2 * i + 1, 1, later)
            return following

        lax.fori_loop(0, GROUP_WIDTH // 2, two_heads, score(0, 0))
        for half in range(2):
            lanes = pl.ds(half * HALF, HALF)
            put_stats(part.at[where, kind, half], tops[:, lanes], sums[:, lanes])

    def put_stats(ref, top, total):
        high = total.astype(jnp.bfloat16).astype(jnp.float32)
        stats = jnp.concatenate([top, high, total - high, jnp.zeros_like(top)], axis=0)
        ref[OUT_ROWS:PART_ROWS, :] = stats.astype(jnp.bfloat16)

    def get_stats(ref):
        stats = ref[OUT_ROWS:PART_ROWS, :].astype(jnp.float32)
        return stats[0:8], stats[8:16] + stats[16:24]

    def merge(ref, others):
        pairs = [get_stats(r) for r in [ref] + others]
        top = functools.reduce(jnp.maximum, [p[0] for p in pairs])
        factors = [jnp.exp2(p[0] - top) for p in pairs]
        total = sum(p[1] * f for p, f in zip(pairs, factors))
        for h in range(GROUP_WIDTH):
            rows = slice(h * HEAD_SIZE, (h + 1) * HEAD_SIZE)
            acc = sum(
                r[rows, :].astype(jnp.float32) * f[h : h + 1]
                for r, f in zip([ref] + others, factors)
            )
            ref[rows, :] = acc.astype(jnp.bfloat16)
        put_stats(ref, top, total)

    halves = (0, 1)
    for half in halves:
        for direction in (0, 1):
            q_copy(direction, 1, half).start()
        q_core_copy(0, half).start()
    for dx, dk in peers[1:]:
        table_copy(dx, dk).start()
    fetch_pool.wait()
    fetch_suffix.wait()
    attend(0, 0, True)
    for dx, dk in peers[1:]:
        table_copy(dx, dk).wait_recv()
        place = 2 * ((-dx) % chips) + dk
        load = table_load(place)
        load.start()
        load.wait()

    def arrived(step, direction, half):
        q_copy(direction, step, half).wait_recv()
        if step + 1 < far or (step + 1 == far and half == direction):
            q_copy(direction, step + 1, half).start()
        q_core_copy(-step if direction == 0 else step, half).start()

    def other_core(offset):
        for half in halves:
            q_core_copy(offset, half).wait_recv()
        attend(offset, 1, False)
        p_core_copy(offset).start()

    other_core(0)
    for direction in (0, 1):
        arrived(1, direction, 0)
    for step in range(1, far):
        for direction in (0, 1):
            arrived(step, direction, 1)
        attend(-step, 0, False)
        attend(step, 0, False)
        if step + 1 < far:
            other_core(-step)
            for direction in (0, 1):
                arrived(step + 1, direction, 0)
            other_core(step)
    if far > 1:
        other_core(1 - far)
    arrived(far, 0, 0)
    arrived(far, 1, 1)
    attend(far, 0, False)
    other_core(far)

    p_core_copy(far).wait_recv()
    for direction in (0, 1):
        half = direction
        merge(part.at[far, 0, half], [partner_part.at[far, half]])
        p_copy(direction, far, half).start()
    if far > 1:
        other_core(far - 1)
    for distance in range(far - 1, 0, -1):
        for direction in (0, 1):
            offset = (distance if direction == 0 else -distance) % chips
            p_core_copy(offset).wait_recv()
        for turn in (0, 1):
            for direction in (0, 1):
                offset = (distance if direction == 0 else -distance) % chips
                half = direction if turn == 1 else 1 - direction
                others = [partner_part.at[offset, half]]
                if distance < far - 1 or half == direction:
                    p_copy(direction, distance + 1, half).wait_recv()
                    others.append(ring_in.at[direction, distance, half])
                merge(part.at[offset, 0, half], others)
                p_copy(direction, distance, half).start()
    def mixed_chunk(offset, kind, half):
        return mixed_all.at[offset % chips, kind, pl.ds(half * HALF, HALF), :]

    def m_copy(direction, step, half):
        sign = -1 if direction == 0 else 1
        return pltpu.make_async_remote_copy(
            src_ref=mixed_chunk(sign * (step - 1), 0, half),
            dst_ref=mixed_chunk(sign * step, 0, half),
            send_sem=m_send.at[direction, step - 1, half],
            recv_sem=m_recv.at[direction, step - 1, half],
            device_id=toward[direction],
            device_id_type=MESH,
        )

    def m_core_copy(offset, half):
        return pltpu.make_async_remote_copy(
            src_ref=mixed_chunk(offset, 0, half),
            dst_ref=mixed_chunk(offset, 1, half),
            send_sem=m_core_send.at[offset % chips, half],
            recv_sem=m_core_recv.at[offset % chips, half],
            device_id=partner,
            device_id_type=MESH,
        )

    p_core_copy(0).wait_recv()
    for half in halves:
        for direction in (0, 1):
            p_copy(direction, 1, half).wait_recv()
        refs = [part.at[0, 0, half], partner_part.at[0, half], ring_in.at[0, 0, half], ring_in.at[1, 0, half]]
        pairs = [get_stats(r) for r in refs]
        top = functools.reduce(jnp.maximum, [p[0] for p in pairs])
        factors = [jnp.exp2(p[0] - top) for p in pairs]
        total = sum(p[1] * f for p, f in zip(pairs, factors))
        factors = [f / total for f in factors]
        for h in range(GROUP_WIDTH):
            rows = slice(h * HEAD_SIZE, (h + 1) * HEAD_SIZE)
            acc = sum(r[rows, :].astype(jnp.float32) * f[h : h + 1] for r, f in zip(refs, factors))
            mixed_all[0, 0, half * HALF : (half + 1) * HALF, rows] = acc.T.astype(jnp.bfloat16)
        for direction in (0, 1):
            if far > 1 or half == direction:
                m_copy(direction, 1, half).start()
        m_core_copy(0, half).start()
    fetch_weight.wait()

    def mixed_arrived(step, direction, half):
        m_copy(direction, step, half).wait_recv()
        if step + 1 < far or (step + 1 == far and half == direction):
            m_copy(direction, step + 1, half).start()
        m_core_copy(-step if direction == 0 else step, half).start()

    def t_copy(batch, direction, distance, half):
        index, first, count = batch
        sign = 1 if direction == 0 else -1
        return pltpu.make_async_remote_copy(
            src_ref=terms.at[(sign * distance) % spans, half, pl.ds(first, count)],
            dst_ref=terms_in.at[direction, distance - 1, half, pl.ds(first, count)],
            send_sem=t_send.at[index, direction, distance - 1, half],
            recv_sem=t_recv.at[index, direction, distance - 1, half],
            device_id=toward_span[direction],
            device_id_type=MESH,
        )

    block_rows = terms.shape[3]
    half_columns = terms.shape[4]
    place_rows = pl.ds(pl.multiple_of(y * block_rows, block_rows), block_rows)
    place_columns = pl.ds(pl.multiple_of(lax.rem(me, slabs) * 2 * half_columns, 2 * half_columns), 2 * half_columns)

    def f_copy(slot, offset, kind):
        target = dict(cache_peer(offset % chips, kind), tensor=goal)
        return pltpu.make_async_remote_copy(
            src_ref=finished.at[slot],
            dst_ref=landed.at[place_rows, place_columns],
            send_sem=f_send.at[slot],
            recv_sem=f_recv.at[y, lax.rem(me, slabs)],
            device_id=target,
            device_id_type=MESH,
        )

    def project(slot, offset, kind):
        term = jnp.dot(mixed_all[offset % chips, kind], weight[...], preferred_element_type=jnp.float32)
        low = term.astype(jnp.bfloat16)
        for block in range(spans):
            where = lax.rem(block - y + spans, spans)
            for half in halves:
                terms[where, half, slot] = low[
                    block * block_rows : (block + 1) * block_rows,
                    half * half_columns : (half + 1) * half_columns,
                ]

    def reduce_terms(batch, members):
        index, first, count = batch
        here = pl.ds(first, count)

        def passed_on(direction, distance, half):
            where = (distance if direction == 0 else -distance) % spans
            if distance < far_span - 1 or half == direction:
                t_copy(batch, direction, distance + 1, half).wait_recv()
                terms[where, half, here] = (
                    terms[where, half, here].astype(jnp.float32)
                    + terms_in[direction, distance, half, here].astype(jnp.float32)
                ).astype(jnp.bfloat16)
            t_copy(batch, direction, distance, half).start()

        def finish(half):
            for direction in (0, 1):
                if far_span > 1 or half == direction:
                    t_copy(batch, direction, 1, half).wait_recv()
            total = terms[0, half, here].astype(jnp.float32)
            for direction in (0, 1):
                if far_span > 1 or half == direction:
                    total = total + terms_in[direction, 0, half, here].astype(jnp.float32)
            finished[here, :, half * half_columns : (half + 1) * half_columns] = total.astype(jnp.bfloat16)

        for direction in (0, 1):
            t_copy(batch, direction, far_span, direction).start()
        if far_span > 1:
            for direction in (0, 1):
                passed_on(direction, far_span - 1, 1 - direction)
        yield
        for distance in range(far_span - 1, 0, -1):
            for direction in (0, 1):
                passed_on(direction, distance, direction)
            if distance > 1:
                for direction in (0, 1):
                    passed_on(direction, distance - 1, 1 - direction)
            yield
        for half in halves:
            finish(half)
        for slot, (offset, kind) in enumerate(members, first):
            if offset == 0 and kind == 0:

                @pl.when(at_goal)
                def _():
                    landed[place_rows, place_columns] = finished[slot]

                @pl.when(jnp.logical_not(at_goal))
                def _():
                    f_copy(slot, offset, kind).start()

            else:
                f_copy(slot, offset, kind).start()

    batches = [[(0, 0), (0, 1)]]
    for step in range(1, far):
        batches.append([(-step, 0), (step, 0), (-step, 1), (step, 1)])
    batches.append([(far, 0), (far, 1)])
    active = []

    def launch(index):
        first = sum(len(b) for b in batches[:index])
        for slot, (offset, kind) in enumerate(batches[index], first):
            if kind == 1:
                for half in halves:
                    m_core_copy(offset, half).wait_recv()
            project(slot, offset, kind)
        active.append(reduce_terms((index, first, len(batches[index])), batches[index]))
        next(active[-1])

    def advance():
        for item in list(active):
            try:
                next(item)
            except StopIteration:
                active.remove(item)

    launch(0)
    for step in range(1, far):
        for direction in (0, 1):
            mixed_arrived(step, direction, 0)
        advance()
        for direction in (0, 1):
            mixed_arrived(step, direction, 1)
        advance()
        launch(step)
    mixed_arrived(far, 0, 0)
    mixed_arrived(far, 1, 1)
    advance()
    launch(far)
    while active:
        advance()

    for dj in range(slabs):
        for dv in range(spans):

            def take():
                block = lax.rem(y + dv, spans)
                slab = lax.rem(me + dj, slabs)
                pltpu.make_async_remote_copy(
                    src_ref=finished.at[0],
                    dst_ref=landed.at[place_rows, place_columns],
                    send_sem=f_send.at[0],
                    recv_sem=f_recv.at[block, slab],
                    device_id=partner,
                    device_id_type=MESH,
                ).wait_recv()

            if dj == 0 and dv == 0:
                pl.when(jnp.logical_not(at_goal))(take)
            else:
                take()
    store = pltpu.make_async_copy(landed, out_hbm, local_sem.at[6])
    store.start()

    for direction in (0, 1):
        for half in halves:
            for step in range(1, far + 1):
                if step < far or half == direction:
                    q_copy(direction, step, half).wait_send()
                    p_copy(direction, step, half).wait_send()
                    m_copy(direction, step, half).wait_send()
            for step in range(1, far_span + 1):
                if step < far_span or half == direction:
                    first = 0
                    for index, members in enumerate(batches):
                        t_copy((index, first, len(members)), direction, step, half).wait_send()
                        first += len(members)
    for offset in range(chips):
        for half in halves:
            q_core_copy(offset, half).wait_send()
            m_core_copy(offset, half).wait_send()
        p_core_copy(offset).wait_send()
    for dx, dk in peers[1:]:
        table_copy(dx, dk).wait_send()
    slot = 0
    for members in batches:
        for offset, kind in members:
            if slot == 0:

                @pl.when(jnp.logical_not(at_goal))
                def _():
                    f_copy(0, 0, 0).wait_send()

            else:
                f_copy(slot, offset, kind).wait_send()
            slot += 1
    store.wait()


def prefill(table, queries, kv_pages, suffix_key_value, out_weight):
    chips = lax.axis_size("cache_0")
    spans = lax.axis_size("tensor")
    caches = 2 * chips
    capacity = (3 * MAXP + 2 * caches - 1) // (2 * caches)
    far = chips // 2
    far_span = spans // 2
    long = capacity * PAGE_TOKENS + SUF
    width = out_weight.shape[1]
    bf16 = jnp.bfloat16
    any_space = pl.BlockSpec(memory_space=pl.ANY)
    flops = 4 * caches * GROUP_WIDTH * SUF * HEAD_SIZE * capacity * PAGE_TOKENS
    dma = pltpu.SemaphoreType.DMA
    out_shape = (SUF, width * caches // spans)
    return pl.pallas_call(
        functools.partial(prefill_kernel, capacity, chips, spans),
        out_shape=jax.ShapeDtypeStruct(out_shape, bf16),
        in_specs=[pl.BlockSpec(memory_space=pltpu.SMEM)] + [any_space] * 5,
        out_specs=any_space,
        scratch_shapes=[
            pltpu.VMEM(kv_pages.shape, bf16),
            pltpu.VMEM(suffix_key_value.shape, bf16),
            pltpu.VMEM(out_weight.shape, bf16),
            pltpu.VMEM((chips, 2) + queries.shape, bf16),
            pltpu.VMEM((chips, 2, 2, PART_ROWS, HALF), bf16),
            pltpu.VMEM((chips, 2, PART_ROWS, HALF), bf16),
            pltpu.VMEM((2, far, 2, PART_ROWS, HALF), bf16),
            pltpu.VMEM((long, HEAD_SIZE), bf16),
            pltpu.VMEM((VALUE_ROWS, long), bf16),
            pltpu.VMEM((2, long, SUF), jnp.float32),
            pltpu.VMEM((2, long, SUF), bf16),
            pltpu.VMEM((GROUP_WIDTH, SUF), jnp.float32),
            pltpu.VMEM((GROUP_WIDTH, SUF), jnp.float32),
            pltpu.SMEM((caches,) + table.shape, jnp.int32),
            pltpu.VMEM((caches,) + table.shape, jnp.int32),
            pltpu.VMEM((chips, 2) + queries.shape, bf16),
            pltpu.VMEM((spans, 2, caches, SUF // spans, width // 2), bf16),
            pltpu.VMEM((2, far_span, 2, caches, SUF // spans, width // 2), bf16),
            pltpu.VMEM((caches, SUF // spans, width), bf16),
            pltpu.VMEM(out_shape, bf16),
            dma((7,)),
            dma((caches,)),
            dma((caches,)),
            dma((2, far, 2)),
            dma((2, far, 2)),
            dma((chips, 2)),
            dma((chips, 2)),
            dma((chips,)),
            dma((chips,)),
            dma((2, far, 2)),
            dma((2, far, 2)),
            dma((2, far, 2)),
            dma((2, far, 2)),
            dma((chips, 2)),
            dma((chips, 2)),
            dma((far + 1, 2, far_span, 2)),
            dma((far + 1, 2, far_span, 2)),
            dma((caches,)),
            dma((spans, caches // spans)),
        ],
        compiler_params=pltpu.CompilerParams(
            collective_id=0, has_side_effects=True, vmem_limit_bytes=62 * 1024 * 1024
        ),
        cost_estimate=pl.CostEstimate(
            flops=flops, bytes_accessed=kv_pages.size * 2, transcendentals=0
        ),
        name="prefill",
    )(table, table, queries, kv_pages, suffix_key_value, out_weight)


def slot_tables(kv_pages, page_ids, prefix_pages, page_home):
    cache_count = lax.axis_size(CACHE)
    request_count = page_ids.shape[0]
    capacity = (3 * request_count * MAXP + 2 * cache_count - 1) // (2 * cache_count)
    pool_rows = kv_pages.shape[0]
    table_index = jnp.arange(page_home.shape[0], dtype=jnp.int32)
    owner_index = jnp.arange(cache_count, dtype=jnp.int32)
    buffer_index = jnp.arange(cache_count * capacity, dtype=jnp.int32)
    flat_ids = page_ids.reshape(-1)
    rows_of = jnp.sum(
        jnp.where(flat_ids[:, None] == table_index[None, :], page_home[None, :], 0), axis=1
    )
    owners = rows_of // pool_rows
    within = rows_of % pool_rows
    live_slots = (jnp.arange(MAXP, dtype=jnp.int32)[None, :] < prefix_pages[:, None]).reshape(-1)
    member = ((owners[:, None] == owner_index[None, :]) & live_slots[:, None]).astype(jnp.int32)
    earlier = jnp.cumsum(member, axis=0) - member
    rank_within = jnp.sum(earlier * member, axis=1)
    target = jnp.where(live_slots, owners * capacity + rank_within, -1)
    wanted = jnp.sum(
        jnp.where(target[:, None] == buffer_index[None, :], within[:, None] + 1, 0), axis=0
    )
    lanes = 128 * ((wanted.shape[0] + 127) // 128)
    return jnp.pad(wanted, (0, lanes - wanted.shape[0]))[None, :]


def per_device(queries, suffix_key_value, kv_pages, page_ids, prefix_pages, page_home, out_weight):
    table = slot_tables(kv_pages, page_ids, prefix_pages, page_home)
    return prefill(table, queries, kv_pages, suffix_key_value, out_weight)


def solution(mesh):
    cores = 2
    chips = mesh.shape["cache"] // cores
    split = Mesh(
        mesh.devices.reshape(mesh.shape["groups"], chips, cores, mesh.shape["tensor"]),
        ("groups", "cache_0", "cache_1", "tensor"),
    )
    placed = (
        P(GROUPS_CACHE, "tensor"),
        P(None, GROUPS_CACHE, "tensor"),
        P(GROUPS_CACHE, None, None, "tensor"),
        P(GROUPS_CACHE, None),
        P(GROUPS_CACHE),
        P("groups"),
        P("tensor", CACHE),
    )
    return jax.shard_map(
        per_device,
        mesh=split,
        in_specs=placed,
        out_specs=P(GROUPS_CACHE, "tensor"),
        check_vma=False,
    )
```

```python
import functools

import jax
import jax.numpy as jnp
from jax import lax
from jax.experimental import pallas as pl
from jax.experimental.pallas import tpu as pltpu
from jax.sharding import Mesh
from jax.sharding import PartitionSpec as P

QUERY_HEADS = 64
KEY_VALUE_HEADS = 8
HEAD_SIZE = 128
PAGE_TOKENS = 128
SUF = 256
MAXP = 64
CACHE = ("cache_0", "cache_1")
GROUPS_CACHE = ("groups", "cache_0", "cache_1")
GROUP_WIDTH = QUERY_HEADS // KEY_VALUE_HEADS

LOG2_SCALE = HEAD_SIZE ** (-0.5) * 1.4426950408889634
DEAD = 1e30
HALF = SUF // 2
OUT_ROWS = GROUP_WIDTH * HEAD_SIZE
PART_ROWS = OUT_ROWS + 32
VALUE_ROWS = HEAD_SIZE + 16
MESH = pl.DeviceIdType.MESH


def prefill_kernel(
    capacity,
    chips,
    spans,
    own_table,
    table_hbm,
    q_hbm,
    kv_hbm,
    suffix_hbm,
    weight_hbm,
    out_hbm,
    pool,
    suffix,
    weight,
    q_all,
    part,
    partner_part,
    ring_in,
    keys,
    values_t,
    scores,
    weights,
    tops,
    sums,
    tables,
    tables_in,
    mixed_all,
    terms,
    terms_in,
    finished,
    landed,
    local_sem,
    table_send,
    table_recv,
    q_send,
    q_recv,
    q_core_send,
    q_core_recv,
    p_core_send,
    p_core_recv,
    p_send,
    p_recv,
    m_send,
    m_recv,
    m_core_send,
    m_core_recv,
    t_send,
    t_recv,
    f_send,
    f_recv,
):
    x = lax.axis_index("cache_0")
    core = lax.axis_index("cache_1")
    y = lax.axis_index("tensor")
    me = 2 * x + core
    caches = 2 * chips
    slabs = caches // spans
    goal = me // slabs
    at_goal = goal == y
    right = {"cache_0": lax.rem(x + 1, chips), "cache_1": core}
    left = {"cache_0": lax.rem(x + chips - 1, chips), "cache_1": core}
    partner = {"cache_0": x, "cache_1": 1 - core}
    up = {"tensor": lax.rem(y + 1, spans)}
    down = {"tensor": lax.rem(y + spans - 1, spans)}
    far = chips // 2
    far_span = spans // 2
    toward = (right, left)
    toward_span = (up, down)
    peers = [(dx, dk) for dx in range(chips) for dk in (0, 1)]

    def cache_peer(dx, dk):
        return {"cache_0": lax.rem(x + dx, chips), "cache_1": core if dk == 0 else 1 - core}

    def source_peer(dj, dv):
        cache = y * slabs + lax.rem(me + dj, slabs)
        return {"cache_0": cache // 2, "cache_1": lax.rem(cache, 2), "tensor": lax.rem(y + dv, spans)}

    fetch_q = pltpu.make_async_copy(q_hbm, q_all.at[0, 0], local_sem.at[0])
    fetch_table = pltpu.make_async_copy(table_hbm, tables_in.at[0], local_sem.at[1])
    fetch_pool = pltpu.make_async_copy(kv_hbm, pool, local_sem.at[2])
    fetch_suffix = pltpu.make_async_copy(suffix_hbm, suffix, local_sem.at[3])
    fetch_weight = pltpu.make_async_copy(weight_hbm, weight, local_sem.at[4])
    fetch_q.start()
    fetch_table.start()
    fetch_pool.start()
    fetch_suffix.start()
    fetch_weight.start()
    barrier = pltpu.get_barrier_semaphore()
    for dx, dk in peers[1:]:
        pl.semaphore_signal(barrier, inc=1, device_id=cache_peer(dx, dk), device_id_type=MESH)
    for peer in toward_span:
        pl.semaphore_signal(barrier, inc=1, device_id=peer, device_id_type=MESH)
    for dj in range(slabs):
        for dv in range(spans):
            pl.semaphore_signal(barrier, inc=1, device_id=source_peer(dj, dv), device_id_type=MESH)
    values_t[HEAD_SIZE:, :] = jnp.ones((VALUE_ROWS - HEAD_SIZE, values_t.shape[1]), jnp.bfloat16)
    fetch_q.wait()
    fetch_table.wait()
    pl.semaphore_wait(barrier, caches - 1 + 2 + caches)

    def chunk(offset, kind, half):
        return q_all.at[offset % chips, kind, pl.ds(half * HALF, HALF), :]

    def q_copy(direction, step, half):
        sign = -1 if direction == 0 else 1
        return pltpu.make_async_remote_copy(
            src_ref=chunk(sign * (step - 1), 0, half),
            dst_ref=chunk(sign * step, 0, half),
            send_sem=q_send.at[direction, step - 1, half],
            recv_sem=q_recv.at[direction, step - 1, half],
            device_id=toward[direction],
            device_id_type=MESH,
        )

    def q_core_copy(offset, half):
        return pltpu.make_async_remote_copy(
            src_ref=chunk(offset, 0, half),
            dst_ref=chunk(offset, 1, half),
            send_sem=q_core_send.at[offset % chips, half],
            recv_sem=q_core_recv.at[offset % chips, half],
            device_id=partner,
            device_id_type=MESH,
        )

    def p_core_copy(offset):
        return pltpu.make_async_remote_copy(
            src_ref=part.at[offset % chips, 1],
            dst_ref=partner_part.at[offset % chips],
            send_sem=p_core_send.at[offset % chips],
            recv_sem=p_core_recv.at[offset % chips],
            device_id=partner,
            device_id_type=MESH,
        )

    def table_copy(dx, dk):
        place = 2 * ((-dx) % chips) + dk
        return pltpu.make_async_remote_copy(
            src_ref=tables_in.at[0],
            dst_ref=tables_in.at[place],
            send_sem=table_send.at[place],
            recv_sem=table_recv.at[place],
            device_id=cache_peer(dx, dk),
            device_id_type=MESH,
        )

    table_load = pltpu.make_async_copy(tables_in, tables, local_sem.at[5])

    def p_copy(direction, distance, half):
        sign = 1 if direction == 0 else -1
        return pltpu.make_async_remote_copy(
            src_ref=part.at[(sign * distance) % chips, 0, half],
            dst_ref=ring_in.at[direction, distance - 1, half],
            send_sem=p_send.at[direction, distance - 1, half],
            recv_sem=p_recv.at[direction, distance - 1, half],
            device_id=toward[direction],
            device_id_type=MESH,
        )

    def attend(offset, kind, own):
        where = offset % chips
        place = 2 * where + kind
        pages = capacity + (SUF // PAGE_TOKENS if own else 0)
        alive = []
        for j in range(capacity):
            if own:
                entry = own_table[0, me * capacity + j]
            else:
                entry = tables[place, 0, me * capacity + j]
            row = jnp.maximum(entry - 1, 0)
            alive.append(jnp.minimum(entry, 1).astype(jnp.float32))
            keys[j * PAGE_TOKENS : (j + 1) * PAGE_TOKENS, :] = pool[row, 0]
            values_t[0:HEAD_SIZE, j * PAGE_TOKENS : (j + 1) * PAGE_TOKENS] = pool[row, 1].T
        if own:
            keys[capacity * PAGE_TOKENS :, :] = suffix[0]
            values_t[0:HEAD_SIZE, capacity * PAGE_TOKENS :] = suffix[1].T

        length = pages * PAGE_TOKENS

        def score(h, slot):
            q_head = q_all[where, kind, :, pl.ds(pl.multiple_of(h * HEAD_SIZE, HEAD_SIZE), HEAD_SIZE)]
            top = None
            for j in range(pages):
                span = pl.ds(j * PAGE_TOKENS, PAGE_TOKENS)
                piece = lax.dot_general(
                    keys[span, :], q_head, (((1,), (1,)), ((), ())), preferred_element_type=jnp.float32
                )
                if j >= capacity:
                    key_at = lax.broadcasted_iota(jnp.int32, piece.shape, 0) + (j - capacity) * PAGE_TOKENS
                    token_at = lax.broadcasted_iota(jnp.int32, piece.shape, 1)
                    piece = jnp.where(key_at <= token_at, piece, -DEAD)
                scores[slot, span, :] = piece
                peak = jnp.max(piece, axis=0, keepdims=True)
                if j < capacity:
                    peak = peak * alive[j] + (alive[j] - 1.0) * DEAD
                top = peak if top is None else jnp.maximum(top, peak)
            return jnp.ceil(top * (LOG2_SCALE * 0.25)) * 4.0

        def gather_values(h, slot, level):
            for j in range(pages):
                span = pl.ds(j * PAGE_TOKENS, PAGE_TOKENS)
                shift = -level
                if j < capacity:
                    shift = shift * alive[j] + (alive[j] - 1.0) * DEAD
                weights[slot, span, :] = jnp.exp2(scores[slot, span, :] * LOG2_SCALE + shift).astype(jnp.bfloat16)
            mixed = jnp.dot(values_t[:, 0:length], weights[slot, 0:length, :], preferred_element_type=jnp.float32)
            rows = pl.ds(pl.multiple_of(h * HEAD_SIZE, HEAD_SIZE), HEAD_SIZE)
            low = mixed[0:HEAD_SIZE].astype(jnp.bfloat16)
            part[where, kind, 0, rows, :] = low[:, 0:HALF]
            part[where, kind, 1, rows, :] = low[:, HALF:]
            tops[pl.ds(h, 1), :] = level
            sums[pl.ds(h, 1), :] = mixed[HEAD_SIZE : HEAD_SIZE + 1]

        def two_heads(i, level):
            later = score(2 * i + 1, 1)
            gather_values(2 * i, 0, level)
            following = score(jnp.minimum(2 * i + 2, GROUP_WIDTH - 1), 0)
            gather_values(2 * i + 1, 1, later)
            return following

        lax.fori_loop(0, GROUP_WIDTH // 2, two_heads, score(0, 0))
        for half in range(2):
            lanes = pl.ds(half * HALF, HALF)
            put_stats(part.at[where, kind, half], tops[:, lanes], sums[:, lanes])

    def put_stats(ref, top, total):
        high = total.astype(jnp.bfloat16).astype(jnp.float32)
        stats = jnp.concatenate([top, high, total - high, jnp.zeros_like(top)], axis=0)
        ref[OUT_ROWS:PART_ROWS, :] = stats.astype(jnp.bfloat16)

    def get_stats(ref):
        stats = ref[OUT_ROWS:PART_ROWS, :].astype(jnp.float32)
        return stats[0:8], stats[8:16] + stats[16:24]

    def merge(ref, others):
        pairs = [get_stats(r) for r in [ref] + others]
        top = functools.reduce(jnp.maximum, [p[0] for p in pairs])
        factors = [jnp.exp2(p[0] - top) for p in pairs]
        total = sum(p[1] * f for p, f in zip(pairs, factors))
        for h in range(GROUP_WIDTH):
            rows = slice(h * HEAD_SIZE, (h + 1) * HEAD_SIZE)
            acc = sum(
                r[rows, :].astype(jnp.float32) * f[h : h + 1]
                for r, f in zip([ref] + others, factors)
            )
            ref[rows, :] = acc.astype(jnp.bfloat16)
        put_stats(ref, top, total)

    halves = (0, 1)
    for half in halves:
        for direction in (0, 1):
            q_copy(direction, 1, half).start()
        q_core_copy(0, half).start()
    for dx, dk in peers[1:]:
        table_copy(dx, dk).start()
    fetch_pool.wait()
    fetch_suffix.wait()
    attend(0, 0, True)
    for dx, dk in peers[1:]:
        table_copy(dx, dk).wait_recv()
    table_load.start()
    table_load.wait()

    def arrived(step, direction, half):
        q_copy(direction, step, half).wait_recv()
        if step + 1 < far or (step + 1 == far and half == direction):
            q_copy(direction, step + 1, half).start()
        q_core_copy(-step if direction == 0 else step, half).start()

    def other_core(offset):
        for half in halves:
            q_core_copy(offset, half).wait_recv()
        attend(offset, 1, False)
        p_core_copy(offset).start()

    other_core(0)
    for direction in (0, 1):
        arrived(1, direction, 0)
    for step in range(1, far):
        for direction in (0, 1):
            arrived(step, direction, 1)
        attend(-step, 0, False)
        attend(step, 0, False)
        if step + 1 < far:
            other_core(-step)
            for direction in (0, 1):
                arrived(step + 1, direction, 0)
            other_core(step)
    if far > 1:
        other_core(1 - far)
        arrived(far, 0, 0)
        arrived(far, 1, 1)
        other_core(far - 1)
    else:
        arrived(far, 0, 0)
        arrived(far, 1, 1)
    attend(far, 0, False)

    def pass_on(direction, distance, half):
        offset = (distance if direction == 0 else -distance) % chips
        others = [partner_part.at[offset, half]]
        if distance < far - 1 or (distance == far - 1 and half == direction):
            p_copy(direction, distance + 1, half).wait_recv()
            others.append(ring_in.at[direction, distance, half])
        merge(part.at[offset, 0, half], others)
        p_copy(direction, distance, half).start()

    if far > 1:
        for direction in (0, 1):
            p_core_copy(far - 1 if direction == 0 else 1 - far).wait_recv()
        for direction in (0, 1):
            pass_on(direction, far - 1, 1 - direction)
    other_core(far)
    p_core_copy(far).wait_recv()
    for direction in (0, 1):
        pass_on(direction, far, direction)
    for distance in range(far - 1, 0, -1):
        if distance < far - 1:
            for direction in (0, 1):
                p_core_copy(distance if direction == 0 else -distance).wait_recv()
            for direction in (0, 1):
                pass_on(direction, distance, 1 - direction)
        for direction in (0, 1):
            pass_on(direction, distance, direction)

    def mixed_chunk(offset, kind, half):
        return mixed_all.at[offset % chips, kind, pl.ds(half * HALF, HALF), :]

    def m_copy(direction, step, half):
        sign = -1 if direction == 0 else 1
        return pltpu.make_async_remote_copy(
            src_ref=mixed_chunk(sign * (step - 1), 0, half),
            dst_ref=mixed_chunk(sign * step, 0, half),
            send_sem=m_send.at[direction, step - 1, half],
            recv_sem=m_recv.at[direction, step - 1, half],
            device_id=toward[direction],
            device_id_type=MESH,
        )

    def m_core_copy(offset, half):
        return pltpu.make_async_remote_copy(
            src_ref=mixed_chunk(offset, 0, half),
            dst_ref=mixed_chunk(offset, 1, half),
            send_sem=m_core_send.at[offset % chips, half],
            recv_sem=m_core_recv.at[offset % chips, half],
            device_id=partner,
            device_id_type=MESH,
        )

    p_core_copy(0).wait_recv()
    for half in halves:
        others = [partner_part.at[0, half]]
        if far > 1:
            p_copy(1 - half, 1, half).wait_recv()
            others.append(ring_in.at[1 - half, 0, half])
        merge(part.at[0, 0, half], others)
    for half in halves:
        p_copy(half, 1, half).wait_recv()
        refs = [part.at[0, 0, half], ring_in.at[half, 0, half]]
        pairs = [get_stats(r) for r in refs]
        top = functools.reduce(jnp.maximum, [p[0] for p in pairs])
        factors = [jnp.exp2(p[0] - top) for p in pairs]
        total = sum(p[1] * f for p, f in zip(pairs, factors))
        factors = [f / total for f in factors]
        for h in range(GROUP_WIDTH):
            rows = slice(h * HEAD_SIZE, (h + 1) * HEAD_SIZE)
            acc = sum(r[rows, :].astype(jnp.float32) * f[h : h + 1] for r, f in zip(refs, factors))
            mixed_all[0, 0, half * HALF : (half + 1) * HALF, rows] = acc.T.astype(jnp.bfloat16)
        for direction in (0, 1):
            if far > 1 or half == direction:
                m_copy(direction, 1, half).start()
        m_core_copy(0, half).start()
    fetch_weight.wait()

    def mixed_arrived(step, direction, half):
        m_copy(direction, step, half).wait_recv()
        if step + 1 < far or (step + 1 == far and half == direction):
            m_copy(direction, step + 1, half).start()
        m_core_copy(-step if direction == 0 else step, half).start()

    def t_copy(batch, direction, distance, half):
        index, first, count = batch
        sign = 1 if direction == 0 else -1
        return pltpu.make_async_remote_copy(
            src_ref=terms.at[(sign * distance) % spans, half, pl.ds(first, count)],
            dst_ref=terms_in.at[direction, distance - 1, half, pl.ds(first, count)],
            send_sem=t_send.at[index, direction, distance - 1, half],
            recv_sem=t_recv.at[index, direction, distance - 1, half],
            device_id=toward_span[direction],
            device_id_type=MESH,
        )

    block_rows = terms.shape[3]
    half_columns = terms.shape[4]
    place_rows = pl.ds(pl.multiple_of(y * block_rows, block_rows), block_rows)
    place_columns = pl.ds(pl.multiple_of(lax.rem(me, slabs) * 2 * half_columns, 2 * half_columns), 2 * half_columns)

    def f_copy(slot, offset, kind):
        target = dict(cache_peer(offset % chips, kind), tensor=goal)
        return pltpu.make_async_remote_copy(
            src_ref=finished.at[slot],
            dst_ref=landed.at[place_rows, place_columns],
            send_sem=f_send.at[slot],
            recv_sem=f_recv.at[y, lax.rem(me, slabs)],
            device_id=target,
            device_id_type=MESH,
        )

    def project(slot, offset, kind):
        term = jnp.dot(mixed_all[offset % chips, kind], weight[...], preferred_element_type=jnp.float32)
        low = term.astype(jnp.bfloat16)
        for block in range(spans):
            where = lax.rem(block - y + spans, spans)
            for half in halves:
                terms[where, half, slot] = low[
                    block * block_rows : (block + 1) * block_rows,
                    half * half_columns : (half + 1) * half_columns,
                ]

    def reduce_terms(batch, members):
        index, first, count = batch
        here = pl.ds(first, count)

        def passed_on(direction, distance, half):
            where = (distance if direction == 0 else -distance) % spans
            if distance < far_span - 1 or half == direction:
                t_copy(batch, direction, distance + 1, half).wait_recv()
                terms[where, half, here] = (
                    terms[where, half, here].astype(jnp.float32)
                    + terms_in[direction, distance, half, here].astype(jnp.float32)
                ).astype(jnp.bfloat16)
            t_copy(batch, direction, distance, half).start()

        def finish(half):
            for direction in (0, 1):
                if far_span > 1 or half == direction:
                    t_copy(batch, direction, 1, half).wait_recv()
            total = terms[0, half, here].astype(jnp.float32)
            for direction in (0, 1):
                if far_span > 1 or half == direction:
                    total = total + terms_in[direction, 0, half, here].astype(jnp.float32)
            finished[here, :, half * half_columns : (half + 1) * half_columns] = total.astype(jnp.bfloat16)

        for direction in (0, 1):
            t_copy(batch, direction, far_span, direction).start()
        if far_span > 1:
            for direction in (0, 1):
                passed_on(direction, far_span - 1, 1 - direction)
        yield
        for distance in range(far_span - 1, 0, -1):
            for direction in (0, 1):
                passed_on(direction, distance, direction)
            if distance > 1:
                for direction in (0, 1):
                    passed_on(direction, distance - 1, 1 - direction)
            yield
        for half in halves:
            finish(half)
        for slot, (offset, kind) in enumerate(members, first):
            if offset == 0 and kind == 0:

                @pl.when(at_goal)
                def _():
                    landed[place_rows, place_columns] = finished[slot]

                @pl.when(jnp.logical_not(at_goal))
                def _():
                    f_copy(slot, offset, kind).start()

            else:
                f_copy(slot, offset, kind).start()

    batches = [[(0, 0), (0, 1)]]
    for step in range(1, far):
        batches.append([(-step, 0), (step, 0), (-step, 1), (step, 1)])
    batches.append([(far, 0), (far, 1)])
    active = []

    def launch(index):
        first = sum(len(b) for b in batches[:index])
        for slot, (offset, kind) in enumerate(batches[index], first):
            if kind == 1:
                for half in halves:
                    m_core_copy(offset, half).wait_recv()
            project(slot, offset, kind)
        active.append(reduce_terms((index, first, len(batches[index])), batches[index]))
        next(active[-1])

    def advance():
        for item in list(active):
            try:
                next(item)
            except StopIteration:
                active.remove(item)

    launch(0)
    for step in range(1, far):
        for direction in (0, 1):
            mixed_arrived(step, direction, 0)
        advance()
        for direction in (0, 1):
            mixed_arrived(step, direction, 1)
        advance()
        launch(step)
    mixed_arrived(far, 0, 0)
    mixed_arrived(far, 1, 1)
    advance()
    launch(far)
    while active:
        advance()

    for dj in range(slabs):
        for dv in range(spans):

            def take():
                block = lax.rem(y + dv, spans)
                slab = lax.rem(me + dj, slabs)
                pltpu.make_async_remote_copy(
                    src_ref=finished.at[0],
                    dst_ref=landed.at[place_rows, place_columns],
                    send_sem=f_send.at[0],
                    recv_sem=f_recv.at[block, slab],
                    device_id=partner,
                    device_id_type=MESH,
                ).wait_recv()

            if dj == 0 and dv == 0:
                pl.when(jnp.logical_not(at_goal))(take)
            else:
                take()
    store = pltpu.make_async_copy(landed, out_hbm, local_sem.at[6])
    store.start()

    for direction in (0, 1):
        for half in halves:
            for step in range(1, far + 1):
                if step < far or half == direction:
                    q_copy(direction, step, half).wait_send()
                    p_copy(direction, step, half).wait_send()
                    m_copy(direction, step, half).wait_send()
            for step in range(1, far_span + 1):
                if step < far_span or half == direction:
                    first = 0
                    for index, members in enumerate(batches):
                        t_copy((index, first, len(members)), direction, step, half).wait_send()
                        first += len(members)
    for offset in range(chips):
        for half in halves:
            q_core_copy(offset, half).wait_send()
            m_core_copy(offset, half).wait_send()
        p_core_copy(offset).wait_send()
    for dx, dk in peers[1:]:
        table_copy(dx, dk).wait_send()
    slot = 0
    for members in batches:
        for offset, kind in members:
            if slot == 0:

                @pl.when(jnp.logical_not(at_goal))
                def _():
                    f_copy(0, 0, 0).wait_send()

            else:
                f_copy(slot, offset, kind).wait_send()
            slot += 1
    store.wait()


def prefill(table, queries, kv_pages, suffix_key_value, out_weight):
    chips = lax.axis_size("cache_0")
    spans = lax.axis_size("tensor")
    caches = 2 * chips
    capacity = (3 * MAXP + 2 * caches - 1) // (2 * caches)
    far = chips // 2
    far_span = spans // 2
    long = capacity * PAGE_TOKENS + SUF
    width = out_weight.shape[1]
    bf16 = jnp.bfloat16
    any_space = pl.BlockSpec(memory_space=pl.ANY)
    flops = 4 * caches * GROUP_WIDTH * SUF * HEAD_SIZE * capacity * PAGE_TOKENS
    dma = pltpu.SemaphoreType.DMA
    out_shape = (SUF, width * caches // spans)
    return pl.pallas_call(
        functools.partial(prefill_kernel, capacity, chips, spans),
        out_shape=jax.ShapeDtypeStruct(out_shape, bf16),
        in_specs=[pl.BlockSpec(memory_space=pltpu.SMEM)] + [any_space] * 5,
        out_specs=any_space,
        scratch_shapes=[
            pltpu.VMEM(kv_pages.shape, bf16),
            pltpu.VMEM(suffix_key_value.shape, bf16),
            pltpu.VMEM(out_weight.shape, bf16),
            pltpu.VMEM((chips, 2) + queries.shape, bf16),
            pltpu.VMEM((chips, 2, 2, PART_ROWS, HALF), bf16),
            pltpu.VMEM((chips, 2, PART_ROWS, HALF), bf16),
            pltpu.VMEM((2, far, 2, PART_ROWS, HALF), bf16),
            pltpu.VMEM((long, HEAD_SIZE), bf16),
            pltpu.VMEM((VALUE_ROWS, long), bf16),
            pltpu.VMEM((2, long, SUF), jnp.float32),
            pltpu.VMEM((2, long, SUF), bf16),
            pltpu.VMEM((GROUP_WIDTH, SUF), jnp.float32),
            pltpu.VMEM((GROUP_WIDTH, SUF), jnp.float32),
            pltpu.SMEM((caches,) + table.shape, jnp.int32),
            pltpu.VMEM((caches,) + table.shape, jnp.int32),
            pltpu.VMEM((chips, 2) + queries.shape, bf16),
            pltpu.VMEM((spans, 2, caches, SUF // spans, width // 2), bf16),
            pltpu.VMEM((2, far_span, 2, caches, SUF // spans, width // 2), bf16),
            pltpu.VMEM((caches, SUF // spans, width), bf16),
            pltpu.VMEM(out_shape, bf16),
            dma((7,)),
            dma((caches,)),
            dma((caches,)),
            dma((2, far, 2)),
            dma((2, far, 2)),
            dma((chips, 2)),
            dma((chips, 2)),
            dma((chips,)),
            dma((chips,)),
            dma((2, far, 2)),
            dma((2, far, 2)),
            dma((2, far, 2)),
            dma((2, far, 2)),
            dma((chips, 2)),
            dma((chips, 2)),
            dma((far + 1, 2, far_span, 2)),
            dma((far + 1, 2, far_span, 2)),
            dma((caches,)),
            dma((spans, caches // spans)),
        ],
        compiler_params=pltpu.CompilerParams(
            collective_id=0, has_side_effects=True, vmem_limit_bytes=62 * 1024 * 1024
        ),
        cost_estimate=pl.CostEstimate(
            flops=flops, bytes_accessed=kv_pages.size * 2, transcendentals=0
        ),
        name="prefill",
    )(table, table, queries, kv_pages, suffix_key_value, out_weight)


def slot_tables(kv_pages, page_ids, prefix_pages, page_home):
    cache_count = lax.axis_size(CACHE)
    request_count = page_ids.shape[0]
    capacity = (3 * request_count * MAXP + 2 * cache_count - 1) // (2 * cache_count)
    pool_rows = kv_pages.shape[0]
    table_index = jnp.arange(page_home.shape[0], dtype=jnp.int32)
    owner_index = jnp.arange(cache_count, dtype=jnp.int32)
    buffer_index = jnp.arange(cache_count * capacity, dtype=jnp.int32)
    flat_ids = page_ids.reshape(-1)
    rows_of = jnp.sum(
        jnp.where(flat_ids[:, None] == table_index[None, :], page_home[None, :], 0), axis=1
    )
    owners = rows_of // pool_rows
    within = rows_of % pool_rows
    live_slots = (jnp.arange(MAXP, dtype=jnp.int32)[None, :] < prefix_pages[:, None]).reshape(-1)
    member = ((owners[:, None] == owner_index[None, :]) & live_slots[:, None]).astype(jnp.int32)
    earlier = jnp.cumsum(member, axis=0) - member
    rank_within = jnp.sum(earlier * member, axis=1)
    target = jnp.where(live_slots, owners * capacity + rank_within, -1)
    wanted = jnp.sum(
        jnp.where(target[:, None] == buffer_index[None, :], within[:, None] + 1, 0), axis=0
    )
    lanes = 128 * ((wanted.shape[0] + 127) // 128)
    return jnp.pad(wanted, (0, lanes - wanted.shape[0]))[None, :]


def per_device(queries, suffix_key_value, kv_pages, page_ids, prefix_pages, page_home, out_weight):
    table = slot_tables(kv_pages, page_ids, prefix_pages, page_home)
    return prefill(table, queries, kv_pages, suffix_key_value, out_weight)


def solution(mesh):
    cores = 2
    chips = mesh.shape["cache"] // cores
    split = Mesh(
        mesh.devices.reshape(mesh.shape["groups"], chips, cores, mesh.shape["tensor"]),
        ("groups", "cache_0", "cache_1", "tensor"),
    )
    placed = (
        P(GROUPS_CACHE, "tensor"),
        P(None, GROUPS_CACHE, "tensor"),
        P(GROUPS_CACHE, None, None, "tensor"),
        P(GROUPS_CACHE, None),
        P(GROUPS_CACHE),
        P("groups"),
        P("tensor", CACHE),
    )
    return jax.shard_map(
        per_device,
        mesh=split,
        in_specs=placed,
        out_specs=P(GROUPS_CACHE, "tensor"),
        check_vma=False,
    )
```

```python
import functools

import jax
import jax.numpy as jnp
from jax import lax
from jax.experimental import pallas as pl
from jax.experimental.pallas import tpu as pltpu
from jax.sharding import Mesh
from jax.sharding import PartitionSpec as P

QUERY_HEADS = 64
KEY_VALUE_HEADS = 8
HEAD_SIZE = 128
PAGE_TOKENS = 128
SUF = 256
MAXP = 64
CACHE = ("cache_0", "cache_1")
GROUPS_CACHE = ("groups", "cache_0", "cache_1")
GROUP_WIDTH = QUERY_HEADS // KEY_VALUE_HEADS

LOG2_SCALE = HEAD_SIZE ** (-0.5) * 1.4426950408889634
DEAD = 1e30
HALF = SUF // 2
OUT_ROWS = GROUP_WIDTH * HEAD_SIZE
PART_ROWS = OUT_ROWS + 32
VALUE_ROWS = HEAD_SIZE + 16
MESH = pl.DeviceIdType.MESH


def prefill_kernel(
    capacity,
    chips,
    spans,
    own_table,
    table_hbm,
    q_hbm,
    kv_hbm,
    suffix_hbm,
    weight_hbm,
    out_hbm,
    pool,
    suffix,
    weight,
    q_all,
    part,
    partner_part,
    ring_in,
    keys,
    values_t,
    scores,
    weights,
    tops,
    sums,
    tables,
    tables_in,
    mixed_all,
    terms,
    terms_in,
    finished,
    landed,
    local_sem,
    table_send,
    table_recv,
    q_send,
    q_recv,
    q_core_send,
    q_core_recv,
    p_core_send,
    p_core_recv,
    p_send,
    p_recv,
    m_send,
    m_recv,
    m_core_send,
    m_core_recv,
    t_send,
    t_recv,
    f_send,
    f_recv,
):
    x = lax.axis_index("cache_0")
    core = lax.axis_index("cache_1")
    y = lax.axis_index("tensor")
    me = 2 * x + core
    caches = 2 * chips
    slabs = caches // spans
    goal = me // slabs
    at_goal = goal == y
    right = {"cache_0": lax.rem(x + 1, chips), "cache_1": core}
    left = {"cache_0": lax.rem(x + chips - 1, chips), "cache_1": core}
    partner = {"cache_0": x, "cache_1": 1 - core}
    up = {"tensor": lax.rem(y + 1, spans)}
    down = {"tensor": lax.rem(y + spans - 1, spans)}
    far = chips // 2
    far_span = spans // 2
    toward = (right, left)
    toward_span = (up, down)
    peers = [(dx, dk) for dx in range(chips) for dk in (0, 1)]

    def cache_peer(dx, dk):
        return {"cache_0": lax.rem(x + dx, chips), "cache_1": core if dk == 0 else 1 - core}

    def source_peer(dj, dv):
        cache = y * slabs + lax.rem(me + dj, slabs)
        return {"cache_0": cache // 2, "cache_1": lax.rem(cache, 2), "tensor": lax.rem(y + dv, spans)}

    fetch_q = pltpu.make_async_copy(q_hbm, q_all.at[0, 0], local_sem.at[0])
    fetch_table = pltpu.make_async_copy(table_hbm, tables_in.at[0], local_sem.at[1])
    fetch_pool = pltpu.make_async_copy(kv_hbm, pool, local_sem.at[2])
    fetch_suffix = pltpu.make_async_copy(suffix_hbm, suffix, local_sem.at[3])
    fetch_weight = pltpu.make_async_copy(weight_hbm, weight, local_sem.at[4])
    fetch_q.start()
    fetch_table.start()
    fetch_pool.start()
    fetch_suffix.start()
    fetch_weight.start()
    barrier = pltpu.get_barrier_semaphore()
    for dx, dk in peers[1:]:
        pl.semaphore_signal(barrier, inc=1, device_id=cache_peer(dx, dk), device_id_type=MESH)
    for peer in toward_span:
        pl.semaphore_signal(barrier, inc=1, device_id=peer, device_id_type=MESH)
    for dj in range(slabs):
        for dv in range(spans):
            pl.semaphore_signal(barrier, inc=1, device_id=source_peer(dj, dv), device_id_type=MESH)
    values_t[HEAD_SIZE:, :] = jnp.ones((VALUE_ROWS - HEAD_SIZE, values_t.shape[1]), jnp.bfloat16)
    fetch_q.wait()
    fetch_table.wait()
    pl.semaphore_wait(barrier, caches - 1 + 2 + caches)

    def chunk(offset, kind, half):
        return q_all.at[offset % chips, kind, pl.ds(half * HALF, HALF), :]

    def q_copy(direction, step, half):
        sign = -1 if direction == 0 else 1
        return pltpu.make_async_remote_copy(
            src_ref=chunk(sign * (step - 1), 0, half),
            dst_ref=chunk(sign * step, 0, half),
            send_sem=q_send.at[direction, step - 1, half],
            recv_sem=q_recv.at[direction, step - 1, half],
            device_id=toward[direction],
            device_id_type=MESH,
        )

    def q_core_copy(offset, half):
        return pltpu.make_async_remote_copy(
            src_ref=chunk(offset, 0, half),
            dst_ref=chunk(offset, 1, half),
            send_sem=q_core_send.at[offset % chips, half],
            recv_sem=q_core_recv.at[offset % chips, half],
            device_id=partner,
            device_id_type=MESH,
        )

    def p_core_copy(offset):
        return pltpu.make_async_remote_copy(
            src_ref=part.at[offset % chips, 1],
            dst_ref=partner_part.at[offset % chips],
            send_sem=p_core_send.at[offset % chips],
            recv_sem=p_core_recv.at[offset % chips],
            device_id=partner,
            device_id_type=MESH,
        )

    def table_copy(dx, dk):
        place = 2 * ((-dx) % chips) + dk
        return pltpu.make_async_remote_copy(
            src_ref=tables_in.at[0],
            dst_ref=tables_in.at[place],
            send_sem=table_send.at[place],
            recv_sem=table_recv.at[place],
            device_id=cache_peer(dx, dk),
            device_id_type=MESH,
        )

    table_load = pltpu.make_async_copy(tables_in, tables, local_sem.at[5])

    def p_copy(direction, distance, half):
        sign = 1 if direction == 0 else -1
        return pltpu.make_async_remote_copy(
            src_ref=part.at[(sign * distance) % chips, 0, half],
            dst_ref=ring_in.at[direction, distance - 1, half],
            send_sem=p_send.at[direction, distance - 1, half],
            recv_sem=p_recv.at[direction, distance - 1, half],
            device_id=toward[direction],
            device_id_type=MESH,
        )

    def attend(offset, kind, own):
        where = offset % chips
        place = 2 * where + kind
        pages = capacity + (SUF // PAGE_TOKENS if own else 0)
        alive = []
        for j in range(capacity):
            if own:
                entry = own_table[0, me * capacity + j]
            else:
                entry = tables[place, 0, me * capacity + j]
            row = jnp.maximum(entry - 1, 0)
            alive.append(jnp.minimum(entry, 1).astype(jnp.float32))
            keys[j * PAGE_TOKENS : (j + 1) * PAGE_TOKENS, :] = pool[row, 0]
            values_t[0:HEAD_SIZE, j * PAGE_TOKENS : (j + 1) * PAGE_TOKENS] = pool[row, 1].T
        if own:
            keys[capacity * PAGE_TOKENS :, :] = suffix[0]
            values_t[0:HEAD_SIZE, capacity * PAGE_TOKENS :] = suffix[1].T

        length = pages * PAGE_TOKENS

        def score(h, slot):
            q_head = q_all[where, kind, :, pl.ds(pl.multiple_of(h * HEAD_SIZE, HEAD_SIZE), HEAD_SIZE)]
            top = None
            for j in range(pages):
                span = pl.ds(j * PAGE_TOKENS, PAGE_TOKENS)
                piece = lax.dot_general(
                    keys[span, :], q_head, (((1,), (1,)), ((), ())), preferred_element_type=jnp.float32
                )
                if j >= capacity:
                    key_at = lax.broadcasted_iota(jnp.int32, piece.shape, 0) + (j - capacity) * PAGE_TOKENS
                    token_at = lax.broadcasted_iota(jnp.int32, piece.shape, 1)
                    piece = jnp.where(key_at <= token_at, piece, -DEAD)
                scores[slot, span, :] = piece
                peak = jnp.max(piece, axis=0, keepdims=True)
                if j < capacity:
                    peak = peak * alive[j] + (alive[j] - 1.0) * DEAD
                top = peak if top is None else jnp.maximum(top, peak)
            return jnp.ceil(top * (LOG2_SCALE * 0.25)) * 4.0

        def gather_values(h, slot, level):
            for j in range(pages):
                span = pl.ds(j * PAGE_TOKENS, PAGE_TOKENS)
                shift = -level
                if j < capacity:
                    shift = shift * alive[j] + (alive[j] - 1.0) * DEAD
                weights[slot, span, :] = jnp.exp2(scores[slot, span, :] * LOG2_SCALE + shift).astype(jnp.bfloat16)
            mixed = jnp.dot(values_t[:, 0:length], weights[slot, 0:length, :], preferred_element_type=jnp.float32)
            rows = pl.ds(pl.multiple_of(h * HEAD_SIZE, HEAD_SIZE), HEAD_SIZE)
            low = mixed[0:HEAD_SIZE].astype(jnp.bfloat16)
            part[where, kind, 0, rows, :] = low[:, 0:HALF]
            part[where, kind, 1, rows, :] = low[:, HALF:]
            tops[pl.ds(h, 1), :] = level
            sums[pl.ds(h, 1), :] = mixed[HEAD_SIZE : HEAD_SIZE + 1]

        def two_heads(i, level):
            later = score(2 * i + 1, 1)
            gather_values(2 * i, 0, level)
            following = score(jnp.minimum(2 * i + 2, GROUP_WIDTH - 1), 0)
            gather_values(2 * i + 1, 1, later)
            return following

        lax.fori_loop(0, GROUP_WIDTH // 2, two_heads, score(0, 0))
        for half in range(2):
            lanes = pl.ds(half * HALF, HALF)
            put_stats(part.at[where, kind, half], tops[:, lanes], sums[:, lanes])

    def put_stats(ref, top, total):
        high = total.astype(jnp.bfloat16).astype(jnp.float32)
        stats = jnp.concatenate([top, high, total - high, jnp.zeros_like(top)], axis=0)
        ref[OUT_ROWS:PART_ROWS, :] = stats.astype(jnp.bfloat16)

    def get_stats(ref):
        stats = ref[OUT_ROWS:PART_ROWS, :].astype(jnp.float32)
        return stats[0:8], stats[8:16] + stats[16:24]

    def merge(ref, others):
        pairs = [get_stats(r) for r in [ref] + others]
        top = functools.reduce(jnp.maximum, [p[0] for p in pairs])
        factors = [jnp.exp2(p[0] - top) for p in pairs]
        total = sum(p[1] * f for p, f in zip(pairs, factors))
        for h in range(GROUP_WIDTH):
            rows = slice(h * HEAD_SIZE, (h + 1) * HEAD_SIZE)
            acc = sum(
                r[rows, :].astype(jnp.float32) * f[h : h + 1]
                for r, f in zip([ref] + others, factors)
            )
            ref[rows, :] = acc.astype(jnp.bfloat16)
        put_stats(ref, top, total)

    halves = (0, 1)
    for half in halves:
        for direction in (0, 1):
            q_copy(direction, 1, half).start()
        q_core_copy(0, half).start()
    for dx, dk in peers[1:]:
        table_copy(dx, dk).start()
    fetch_pool.wait()
    fetch_suffix.wait()
    attend(0, 0, True)
    for dx, dk in peers[1:]:
        table_copy(dx, dk).wait_recv()
    table_load.start()
    table_load.wait()

    def arrived(step, direction, half):
        q_copy(direction, step, half).wait_recv()
        if step + 1 < far or (step + 1 == far and half == direction):
            q_copy(direction, step + 1, half).start()
        q_core_copy(-step if direction == 0 else step, half).start()

    def other_core(offset):
        for half in halves:
            q_core_copy(offset, half).wait_recv()
        attend(offset, 1, False)
        p_core_copy(offset).start()

    other_core(0)
    for direction in (0, 1):
        arrived(1, direction, 0)
    for step in range(1, far):
        for direction in (0, 1):
            arrived(step, direction, 1)
        attend(-step, 0, False)
        attend(step, 0, False)
        if step + 1 < far:
            other_core(-step)
            for direction in (0, 1):
                arrived(step + 1, direction, 0)
            other_core(step)
    if far > 1:
        other_core(1 - far)
        arrived(far, 0, 0)
        arrived(far, 1, 1)
        other_core(far - 1)
    else:
        arrived(far, 0, 0)
        arrived(far, 1, 1)
    attend(far, 0, False)

    def pass_on(direction, distance, half):
        offset = (distance if direction == 0 else -distance) % chips
        others = [partner_part.at[offset, half]]
        if distance < far - 1 or (distance == far - 1 and half == direction):
            p_copy(direction, distance + 1, half).wait_recv()
            others.append(ring_in.at[direction, distance, half])
        merge(part.at[offset, 0, half], others)
        p_copy(direction, distance, half).start()

    if far > 1:
        for direction in (0, 1):
            p_core_copy(far - 1 if direction == 0 else 1 - far).wait_recv()
        for direction in (0, 1):
            pass_on(direction, far - 1, 1 - direction)
    other_core(far)
    p_core_copy(far).wait_recv()
    for direction in (0, 1):
        pass_on(direction, far, direction)
    for distance in range(far - 1, 0, -1):
        if distance < far - 1:
            for direction in (0, 1):
                p_core_copy(distance if direction == 0 else -distance).wait_recv()
            for direction in (0, 1):
                pass_on(direction, distance, 1 - direction)
        for direction in (0, 1):
            pass_on(direction, distance, direction)

    def mixed_chunk(offset, kind, half):
        return mixed_all.at[offset % chips, kind, pl.ds(half * HALF, HALF), :]

    def m_copy(direction, step, half):
        sign = -1 if direction == 0 else 1
        return pltpu.make_async_remote_copy(
            src_ref=mixed_chunk(sign * (step - 1), 0, half),
            dst_ref=mixed_chunk(sign * step, 0, half),
            send_sem=m_send.at[direction, step - 1, half],
            recv_sem=m_recv.at[direction, step - 1, half],
            device_id=toward[direction],
            device_id_type=MESH,
        )

    def m_core_copy(offset, half):
        return pltpu.make_async_remote_copy(
            src_ref=mixed_chunk(offset, 0, half),
            dst_ref=mixed_chunk(offset, 1, half),
            send_sem=m_core_send.at[offset % chips, half],
            recv_sem=m_core_recv.at[offset % chips, half],
            device_id=partner,
            device_id_type=MESH,
        )

    p_core_copy(0).wait_recv()
    for half in halves:
        others = [partner_part.at[0, half]]
        if far > 1:
            p_copy(1 - half, 1, half).wait_recv()
            others.append(ring_in.at[1 - half, 0, half])
        merge(part.at[0, 0, half], others)
    for half in halves:
        p_copy(half, 1, half).wait_recv()
        refs = [part.at[0, 0, half], ring_in.at[half, 0, half]]
        pairs = [get_stats(r) for r in refs]
        top = functools.reduce(jnp.maximum, [p[0] for p in pairs])
        factors = [jnp.exp2(p[0] - top) for p in pairs]
        total = sum(p[1] * f for p, f in zip(pairs, factors))
        factors = [f / total for f in factors]
        for h in range(GROUP_WIDTH):
            rows = slice(h * HEAD_SIZE, (h + 1) * HEAD_SIZE)
            acc = sum(r[rows, :].astype(jnp.float32) * f[h : h + 1] for r, f in zip(refs, factors))
            mixed_all[0, 0, half * HALF : (half + 1) * HALF, rows] = acc.T.astype(jnp.bfloat16)
        for direction in (0, 1):
            if far > 1 or half == direction:
                m_copy(direction, 1, half).start()
        m_core_copy(0, half).start()
    fetch_weight.wait()

    def mixed_arrived(step, direction, half):
        m_copy(direction, step, half).wait_recv()
        if step + 1 < far or (step + 1 == far and half == direction):
            m_copy(direction, step + 1, half).start()
        m_core_copy(-step if direction == 0 else step, half).start()

    def t_copy(batch, direction, distance, half):
        index, first, count = batch
        sign = 1 if direction == 0 else -1
        return pltpu.make_async_remote_copy(
            src_ref=terms.at[(sign * distance) % spans, half, pl.ds(first, count)],
            dst_ref=terms_in.at[direction, distance - 1, half, pl.ds(first, count)],
            send_sem=t_send.at[index, direction, distance - 1, half],
            recv_sem=t_recv.at[index, direction, distance - 1, half],
            device_id=toward_span[direction],
            device_id_type=MESH,
        )

    block_rows = terms.shape[3]
    half_columns = terms.shape[4]
    place_rows = pl.ds(pl.multiple_of(y * block_rows, block_rows), block_rows)
    place_columns = pl.ds(pl.multiple_of(lax.rem(me, slabs) * 2 * half_columns, 2 * half_columns), 2 * half_columns)

    def f_copy(slot, offset, kind):
        target = dict(cache_peer(offset % chips, kind), tensor=goal)
        return pltpu.make_async_remote_copy(
            src_ref=finished.at[slot],
            dst_ref=landed.at[place_rows, place_columns],
            send_sem=f_send.at[slot],
            recv_sem=f_recv.at[y, lax.rem(me, slabs)],
            device_id=target,
            device_id_type=MESH,
        )

    def project(slot, offset, kind):
        term = jnp.dot(mixed_all[offset % chips, kind], weight[...], preferred_element_type=jnp.float32)
        low = term.astype(jnp.bfloat16)
        for block in range(spans):
            where = lax.rem(block - y + spans, spans)
            for half in halves:
                terms[where, half, slot] = low[
                    block * block_rows : (block + 1) * block_rows,
                    half * half_columns : (half + 1) * half_columns,
                ]

    def reduce_terms(batch, members):
        index, first, count = batch
        here = pl.ds(first, count)

        def passed_on(direction, distance, half):
            where = (distance if direction == 0 else -distance) % spans
            if distance < far_span - 1 or half == direction:
                t_copy(batch, direction, distance + 1, half).wait_recv()
                terms[where, half, here] = (
                    terms[where, half, here].astype(jnp.float32)
                    + terms_in[direction, distance, half, here].astype(jnp.float32)
                ).astype(jnp.bfloat16)
            t_copy(batch, direction, distance, half).start()

        def finish(half):
            for direction in (0, 1):
                if far_span > 1 or half == direction:
                    t_copy(batch, direction, 1, half).wait_recv()
            total = terms[0, half, here].astype(jnp.float32)
            for direction in (0, 1):
                if far_span > 1 or half == direction:
                    total = total + terms_in[direction, 0, half, here].astype(jnp.float32)
            finished[here, :, half * half_columns : (half + 1) * half_columns] = total.astype(jnp.bfloat16)

        for direction in (0, 1):
            t_copy(batch, direction, far_span, direction).start()
        if far_span > 1:
            for direction in (0, 1):
                passed_on(direction, far_span - 1, 1 - direction)
        yield
        for distance in range(far_span - 1, 0, -1):
            for direction in (0, 1):
                passed_on(direction, distance, direction)
            if distance > 1:
                for direction in (0, 1):
                    passed_on(direction, distance - 1, 1 - direction)
            yield
        for half in halves:
            finish(half)
        for slot, (offset, kind) in enumerate(members, first):
            if offset == 0 and kind == 0:

                @pl.when(at_goal)
                def _():
                    landed[place_rows, place_columns] = finished[slot]

                @pl.when(jnp.logical_not(at_goal))
                def _():
                    f_copy(slot, offset, kind).start()

            else:
                f_copy(slot, offset, kind).start()

    batches = [[(0, 0), (0, 1)]]
    for step in range(1, far):
        batches.append([(-step, 0), (step, 0), (-step, 1), (step, 1)])
    batches.append([(far, 0), (far, 1)])
    active = []

    def launch(index):
        first = sum(len(b) for b in batches[:index])
        for slot, (offset, kind) in enumerate(batches[index], first):
            if kind == 1:
                for half in halves:
                    m_core_copy(offset, half).wait_recv()
            project(slot, offset, kind)
        active.append(reduce_terms((index, first, len(batches[index])), batches[index]))
        next(active[-1])

    def advance(newest_first=False):
        for item in active[::-1] if newest_first else list(active):
            try:
                next(item)
            except StopIteration:
                active.remove(item)

    launch(0)
    for step in range(1, far):
        for direction in (0, 1):
            mixed_arrived(step, direction, 0)
        advance()
        for direction in (0, 1):
            mixed_arrived(step, direction, 1)
        advance()
        launch(step)
    mixed_arrived(far, 0, 0)
    mixed_arrived(far, 1, 1)
    launch(far)
    while active:
        advance(newest_first=True)

    for dj in range(slabs):
        for dv in range(spans):

            def take():
                block = lax.rem(y + dv, spans)
                slab = lax.rem(me + dj, slabs)
                pltpu.make_async_remote_copy(
                    src_ref=finished.at[0],
                    dst_ref=landed.at[place_rows, place_columns],
                    send_sem=f_send.at[0],
                    recv_sem=f_recv.at[block, slab],
                    device_id=partner,
                    device_id_type=MESH,
                ).wait_recv()

            if dj == 0 and dv == 0:
                pl.when(jnp.logical_not(at_goal))(take)
            else:
                take()
    store = pltpu.make_async_copy(landed, out_hbm, local_sem.at[6])
    store.start()

    for direction in (0, 1):
        for half in halves:
            for step in range(1, far + 1):
                if step < far or half == direction:
                    q_copy(direction, step, half).wait_send()
                    p_copy(direction, step, half).wait_send()
                    m_copy(direction, step, half).wait_send()
            for step in range(1, far_span + 1):
                if step < far_span or half == direction:
                    first = 0
                    for index, members in enumerate(batches):
                        t_copy((index, first, len(members)), direction, step, half).wait_send()
                        first += len(members)
    for offset in range(chips):
        for half in halves:
            q_core_copy(offset, half).wait_send()
            m_core_copy(offset, half).wait_send()
        p_core_copy(offset).wait_send()
    for dx, dk in peers[1:]:
        table_copy(dx, dk).wait_send()
    slot = 0
    for members in batches:
        for offset, kind in members:
            if slot == 0:

                @pl.when(jnp.logical_not(at_goal))
                def _():
                    f_copy(0, 0, 0).wait_send()

            else:
                f_copy(slot, offset, kind).wait_send()
            slot += 1
    store.wait()


def prefill(table, queries, kv_pages, suffix_key_value, out_weight):
    chips = lax.axis_size("cache_0")
    spans = lax.axis_size("tensor")
    caches = 2 * chips
    capacity = (3 * MAXP + 2 * caches - 1) // (2 * caches)
    far = chips // 2
    far_span = spans // 2
    long = capacity * PAGE_TOKENS + SUF
    width = out_weight.shape[1]
    bf16 = jnp.bfloat16
    any_space = pl.BlockSpec(memory_space=pl.ANY)
    flops = 4 * caches * GROUP_WIDTH * SUF * HEAD_SIZE * capacity * PAGE_TOKENS
    dma = pltpu.SemaphoreType.DMA
    out_shape = (SUF, width * caches // spans)
    return pl.pallas_call(
        functools.partial(prefill_kernel, capacity, chips, spans),
        out_shape=jax.ShapeDtypeStruct(out_shape, bf16),
        in_specs=[pl.BlockSpec(memory_space=pltpu.SMEM)] + [any_space] * 5,
        out_specs=any_space,
        scratch_shapes=[
            pltpu.VMEM(kv_pages.shape, bf16),
            pltpu.VMEM(suffix_key_value.shape, bf16),
            pltpu.VMEM(out_weight.shape, bf16),
            pltpu.VMEM((chips, 2) + queries.shape, bf16),
            pltpu.VMEM((chips, 2, 2, PART_ROWS, HALF), bf16),
            pltpu.VMEM((chips, 2, PART_ROWS, HALF), bf16),
            pltpu.VMEM((2, far, 2, PART_ROWS, HALF), bf16),
            pltpu.VMEM((long, HEAD_SIZE), bf16),
            pltpu.VMEM((VALUE_ROWS, long), bf16),
            pltpu.VMEM((2, long, SUF), jnp.float32),
            pltpu.VMEM((2, long, SUF), bf16),
            pltpu.VMEM((GROUP_WIDTH, SUF), jnp.float32),
            pltpu.VMEM((GROUP_WIDTH, SUF), jnp.float32),
            pltpu.SMEM((caches,) + table.shape, jnp.int32),
            pltpu.VMEM((caches,) + table.shape, jnp.int32),
            pltpu.VMEM((chips, 2) + queries.shape, bf16),
            pltpu.VMEM((spans, 2, caches, SUF // spans, width // 2), bf16),
            pltpu.VMEM((2, far_span, 2, caches, SUF // spans, width // 2), bf16),
            pltpu.VMEM((caches, SUF // spans, width), bf16),
            pltpu.VMEM(out_shape, bf16),
            dma((7,)),
            dma((caches,)),
            dma((caches,)),
            dma((2, far, 2)),
            dma((2, far, 2)),
            dma((chips, 2)),
            dma((chips, 2)),
            dma((chips,)),
            dma((chips,)),
            dma((2, far, 2)),
            dma((2, far, 2)),
            dma((2, far, 2)),
            dma((2, far, 2)),
            dma((chips, 2)),
            dma((chips, 2)),
            dma((far + 1, 2, far_span, 2)),
            dma((far + 1, 2, far_span, 2)),
            dma((caches,)),
            dma((spans, caches // spans)),
        ],
        compiler_params=pltpu.CompilerParams(
            collective_id=0, has_side_effects=True, vmem_limit_bytes=62 * 1024 * 1024
        ),
        cost_estimate=pl.CostEstimate(
            flops=flops, bytes_accessed=kv_pages.size * 2, transcendentals=0
        ),
        name="prefill",
    )(table, table, queries, kv_pages, suffix_key_value, out_weight)


def slot_tables(kv_pages, page_ids, prefix_pages, page_home):
    cache_count = lax.axis_size(CACHE)
    request_count = page_ids.shape[0]
    capacity = (3 * request_count * MAXP + 2 * cache_count - 1) // (2 * cache_count)
    pool_rows = kv_pages.shape[0]
    table_index = jnp.arange(page_home.shape[0], dtype=jnp.int32)
    owner_index = jnp.arange(cache_count, dtype=jnp.int32)
    buffer_index = jnp.arange(cache_count * capacity, dtype=jnp.int32)
    flat_ids = page_ids.reshape(-1)
    rows_of = jnp.sum(
        jnp.where(flat_ids[:, None] == table_index[None, :], page_home[None, :], 0), axis=1
    )
    owners = rows_of // pool_rows
    within = rows_of % pool_rows
    live_slots = (jnp.arange(MAXP, dtype=jnp.int32)[None, :] < prefix_pages[:, None]).reshape(-1)
    member = ((owners[:, None] == owner_index[None, :]) & live_slots[:, None]).astype(jnp.int32)
    earlier = jnp.cumsum(member, axis=0) - member
    rank_within = jnp.sum(earlier * member, axis=1)
    target = jnp.where(live_slots, owners * capacity + rank_within, -1)
    wanted = jnp.sum(
        jnp.where(target[:, None] == buffer_index[None, :], within[:, None] + 1, 0), axis=0
    )
    lanes = 128 * ((wanted.shape[0] + 127) // 128)
    return jnp.pad(wanted, (0, lanes - wanted.shape[0]))[None, :]


def per_device(queries, suffix_key_value, kv_pages, page_ids, prefix_pages, page_home, out_weight):
    table = slot_tables(kv_pages, page_ids, prefix_pages, page_home)
    return prefill(table, queries, kv_pages, suffix_key_value, out_weight)


def solution(mesh):
    cores = 2
    chips = mesh.shape["cache"] // cores
    split = Mesh(
        mesh.devices.reshape(mesh.shape["groups"], chips, cores, mesh.shape["tensor"]),
        ("groups", "cache_0", "cache_1", "tensor"),
    )
    placed = (
        P(GROUPS_CACHE, "tensor"),
        P(None, GROUPS_CACHE, "tensor"),
        P(GROUPS_CACHE, None, None, "tensor"),
        P(GROUPS_CACHE, None),
        P(GROUPS_CACHE),
        P("groups"),
        P("tensor", CACHE),
    )
    return jax.shard_map(
        per_device,
        mesh=split,
        in_specs=placed,
        out_specs=P(GROUPS_CACHE, "tensor"),
        check_vma=False,
    )
```
